32 devices in a mesh: groups: 2 (over x), tm: 2 (over core), slab: 8 (over z, y).
Axes of the slice: x: 2, y: 2, z: 4, core: 2. Of those that a mesh axis runs over, the one named last changes fastest.
Arguments:
- window_states: float32 [8, 64, 16, 512], P('tm', ('groups', 'slab')), parts along dimension 1, may hold values from -6 to 6
- spatial_weight: bfloat16 [320, 144], replicated, may hold values from -0.5 to 0.5
- temporal_weight: bfloat16 [3, 320, 320], replicated, may hold values from -0.1875 to 0.1875
- out_weight: bfloat16 [16, 320], replicated, may hold values from -0.3125 to 0.3125
- time_embed: float32 [1000, 320], replicated, may hold values from -6 to 6
- step_size: float32 [1000], replicated, may hold values from 0.1 to 0.4
- time_index: int32 [48], P('groups'), parts along dimension 0, may hold values from 0 to 999
- slides: int32 [4], P('groups'), parts along dimension 0, may hold values from 1 to 7
Outputs:
- final_states: float32 [8, 64, 16, 512], P('tm', ('groups', 'slab')), parts along dimension 1
The draws below stay inside these ranges and needn't reach their ends.
There are 2 independent parts, one for each index of `groups`. The reference program is written for one: setup_inputs(seed, part) draws one part's arguments, and reference() takes and returns one part's arrays. A program takes and returns all parts, laid end to end along the dimension named above; an argument that names none is the same for every part. Nothing has to cross between parts.
All inputs are finite; a program needn't handle non-finite values.
Results may differ from the reference program's by a relative error of at most 0.002.
Values may be sent and summed in bfloat16 or wider, within the bound.
No kernel may reach another device: no remote copies, remote signals or barrier semaphores. Data moves between devices by JAX's collectives and lax.ppermute only.
A program may use at most 128 MiB of HBM per device.

```python
import math
import jax
import jax.numpy as jnp
from jax import lax

C = 16
HID = 320
HEIGHT = 16
WIDTH = 32
NSTEPS = 1000
WIN = 8
ITERS = 2
FRAMES = 32
HORIZON = 24


def set_ends(array, key, low, high):
    shape = array.shape
    spot = [jax.random.randint(jax.random.fold_in(key, axis), (), 0, shape[axis]) for axis in range(len(shape))]
    array = array.at[tuple(spot)].set(low)
    longest = shape.index(max(shape))
    spot[longest] = (spot[longest] + 1) % shape[longest]
    return array.at[tuple(spot)].set(high)


def block_scale(own_key, shape, split, least, largest):
    gain = 1.0
    for position, blocks in split:
        draws = jax.random.uniform(jax.random.fold_in(jax.random.fold_in(own_key, 6), position), (blocks,), jnp.float32, least / len(split), largest / len(split))
        gain = gain * jnp.repeat(jnp.exp(draws), shape[position] // blocks).reshape((-1,) + (1,) * (len(shape) - 1 - position))
    return gain


def gaussian(own_key, shape, width, bound, cuts=(), held_as=jnp.bfloat16):
    factor_of = block_scale(own_key, shape, cuts, -0.22, 0.18) if cuts else 1.0
    entries = jax.random.normal(own_key, shape, jnp.float32) * width * factor_of
    return jnp.minimum(jnp.maximum(entries, -bound), bound).astype(held_as)


def setup_inputs(seed: int = 0, part: int = 0) -> dict:
    key_list = jax.random.split(jax.random.key(seed), 9)
    part_splits = jax.random.split(jax.random.fold_in(key_list[8], part), 9)
    window_states = gaussian(part_splits[0], (WIN, FRAMES, C, HEIGHT * WIDTH), 1.0, 6.0, ((0, 2), (1, 8)), jnp.float32)
    spatial_weight = gaussian(key_list[1], (HID, 9 * C), (9 * C) ** -0.5, 0.5)
    temporal_weight = gaussian(key_list[2], (3, HID, HID), (3 * HID) ** -0.5, 0.1875)
    out_weight = gaussian(key_list[3], (C, HID), HID ** -0.5, 0.3125)
    time_embed = gaussian(key_list[4], (NSTEPS, HID), 1.0, 6.0, (), jnp.float32)
    step_size = jnp.clip(jnp.exp(jax.random.uniform(key_list[5], (NSTEPS,), jnp.float32, math.log(0.1), math.log(0.4))), 0.1, 0.4)
    time_index = set_ends(jax.random.randint(part_splits[6], (HORIZON,), 0, NSTEPS), jax.random.fold_in(part_splits[6], 1), 0, NSTEPS - 1).astype(jnp.int32)
    slides = jax.random.randint(part_splits[7], (ITERS,), 1, WIN).astype(jnp.int32)
    return {"window_states": window_states, "spatial_weight": spatial_weight, "temporal_weight": temporal_weight, "out_weight": out_weight, "time_embed": time_embed, "step_size": step_size, "time_index": time_index, "slides": slides}


def drift_one(item, spatial_weight, temporal_weight, out_weight):
    states_one, embed_one = item
    latent = states_one.astype(jnp.bfloat16).reshape(FRAMES, C, HEIGHT, WIDTH)
    padded = jnp.pad(latent, ((0, 0), (0, 0), (1, 1), (1, 1)))
    pieces = []
    for row_shift in range(3):
        for col_shift in range(3):
            pieces.append(padded[:, :, row_shift:row_shift + HEIGHT, col_shift:col_shift + WIDTH])
    columns = jnp.concatenate(pieces, axis=1).reshape(FRAMES, 9 * C, HEIGHT * WIDTH)
    pre = jnp.einsum("oc,fcp->fop", spatial_weight.astype(jnp.float32), columns.astype(jnp.float32))
    pre = pre + embed_one[None, :, None]
    first = jax.nn.silu(pre).astype(jnp.bfloat16)
    framed = jnp.pad(first, ((1, 1), (0, 0), (0, 0)))
    middle = jnp.zeros((FRAMES, HID, HEIGHT * WIDTH), jnp.float32)
    for lagged in range(3):
        middle = middle + jnp.einsum("oc,fcp->fop", temporal_weight[lagged].astype(jnp.float32), framed[lagged:lagged + FRAMES].astype(jnp.float32))
    second = jax.nn.silu(middle).astype(jnp.bfloat16)
    return jnp.einsum("ch,fhp->fcp", out_weight.astype(jnp.float32), second.astype(jnp.float32))


def reference(window_states, spatial_weight, temporal_weight, out_weight, time_embed, step_size, time_index, slides):
    states = window_states
    offset = jnp.zeros((), jnp.int32)
    for sweep in range(ITERS):
        indices = lax.dynamic_slice_in_dim(time_index, offset, WIN)
        embed = time_embed[indices]
        deltas = step_size[indices]
        drifts = lax.map(lambda item: drift_one(item, spatial_weight, temporal_weight, out_weight), (states, embed))
        weighted = deltas[:, None, None, None] * drifts
        running = jnp.cumsum(weighted, axis=0)
        updated = states[0][None] + (running - weighted)
        tail = states[0] + running[-1]
        extended = jnp.concatenate([updated, jnp.broadcast_to(tail[None], updated.shape)], axis=0)
        states = lax.dynamic_slice_in_dim(extended, slides[sweep].astype(jnp.int32), WIN)
        offset = offset + slides[sweep].astype(jnp.int32)
    return states
```

```python
import functools

import jax
import jax.numpy as jnp
from jax import lax
from jax.experimental import pallas as pl
from jax.experimental.pallas import tpu as pltpu
from jax.sharding import PartitionSpec as P

HEIGHT = 16
WIDTH = 32
ITERS = 2
HALO = 2
BF = jnp.bfloat16
F32 = jnp.float32
VMEM = pl.BlockSpec(memory_space=pltpu.VMEM)
SMEM = pl.BlockSpec(memory_space=pltpu.SMEM)
ANY = pl.BlockSpec(memory_space=pl.ANY)


def shape(dims, dtype):
    return jax.ShapeDtypeStruct(dims, dtype)


def prepare(index_ref, slides_ref, states_ref, table_ref, low_ref, high_ref, embed_ref, rows, sems):
    times, frames = states_ref.shape[0], states_ref.shape[1]
    first_time = lax.axis_index("tm") * times
    copies = []
    for sweep in range(ITERS):
        offset = first_time if sweep == 0 else first_time + slides_ref[0]
        for i in range(times):
            slot = sweep * times + i
            row = index_ref[offset + i]
            copy = pltpu.make_async_copy(
                table_ref.at[pl.ds(row, 1)], rows.at[pl.ds(slot, 1)], sems.at[slot]
            )
            copy.start()
            copies.append(copy)
    low_ref[...] = states_ref[:, :HALO].astype(BF)
    high_ref[...] = states_ref[:, frames - HALO :].astype(BF)
    for copy in copies:
        copy.wait()
    embed_ref[...] = rows[...].T


def silu_half(half):
    return half + half * jnp.tanh(half)


def columns_of(latent, lane):
    cells = HEIGHT * WIDTH
    col = lane % WIDTH
    zero = jnp.zeros_like(latent)
    left = jnp.where(col > 0, pltpu.roll(latent, 1, 1), zero)
    right = jnp.where(col < WIDTH - 1, pltpu.roll(latent, cells - 1, 1), zero)
    middle = (left, latent, right)
    above = [jnp.where(lane >= WIDTH, pltpu.roll(x, WIDTH, 1), zero) for x in middle]
    below = [jnp.where(lane < cells - WIDTH, pltpu.roll(x, cells - WIDTH, 1), zero) for x in middle]
    return [*above, *middle, *below]


def one_iteration(
    sweep, low, high, latent_of, valid_of, base_of,
    index_ref, slides_ref, step_ref, spatial_ref, temporal_ref, out_weight_ref, embed_ref,
    own_ref, send_ref, spatial_scr, temporal_scr, first_scr, sums_scr,
):
    times = own_ref.shape[0]
    hidden, taps = spatial_ref.shape
    depth = spatial_scr.shape[1]
    extra = depth - taps
    cells = own_ref.shape[3]
    rank = lax.axis_index("tm")
    lane = lax.broadcasted_iota(jnp.int32, (1, cells), 1)
    for lag in range(3):
        temporal_scr[:, lag * hidden : (lag + 1) * hidden] = (temporal_ref[lag].astype(F32) * 0.5).astype(BF)
    spatial_scr[:, :taps] = (spatial_ref[...].astype(F32) * 0.5).astype(BF)
    for frame in range(low, high):
        sums_scr[0, frame - low] = base_of(frame)
    offset = rank * times + (0 if sweep == 0 else slides_ref[0])
    embed_lane = lax.broadcasted_iota(jnp.int32, (1, embed_ref.shape[1]), 1)
    extra_lane = lax.broadcasted_iota(jnp.int32, (1, extra), 1)

    def conv(t, frame):
        pieces = columns_of(latent_of(t, frame), lane)
        pieces.append(jnp.full((extra, cells), valid_of(frame), F32).astype(BF))
        columns = jnp.concatenate(pieces, axis=0)
        half = jnp.dot(spatial_scr[...], columns, preferred_element_type=F32)
        start = (frame - low + 1) * hidden
        first_scr[start : start + hidden, :] = silu_half(half).astype(BF)

    def temporal(frame):
        start = (frame - low) * hidden
        half = jnp.dot(temporal_scr[...], first_scr[start : start + 3 * hidden, :], preferred_element_type=F32)
        return silu_half(half).astype(BF)

    def project(t, frame, second):
        drift = jnp.dot(out_weight_ref[...], second, preferred_element_type=F32)
        delta = step_ref[index_ref[offset + t]]
        sums_scr[t + 1, frame - low] = sums_scr[t, frame - low] + delta * drift

    def one_time(t, carry):
        picked = jnp.where(embed_lane == sweep * times + t, embed_ref[...], 0.0)
        embed = jnp.sum(picked, axis=1, keepdims=True) * 0.5
        rest = embed
        tail = jnp.zeros((hidden, extra), F32)
        for part in range(3):
            piece = rest.astype(BF).astype(F32)
            tail = jnp.where(extra_lane == part, piece, tail)
            rest = rest - piece
        spatial_scr[:, taps:] = tail.astype(BF)
        conv(t, low - 1)
        conv(t, low)
        waiting = None
        for frame in range(low, high):
            conv(t, frame + 1)
            second = temporal(frame)
            if waiting is not None:
                project(t, *waiting)
            waiting = (frame, second)
        project(t, *waiting)
        return carry

    lax.fori_loop(0, times, one_time, 0)
    slide = slides_ref[sweep]
    for j in range(times):
        own_ref[j] = sums_scr[jnp.minimum(j + slide, times)]
        late = jnp.clip(j + slide - times, 0, times)
        send_ref[j] = sums_scr[jnp.where(rank == 0, times, late)]


def edge_flags():
    slab = lax.axis_index("slab")
    return slab > 0, slab < lax.axis_size("slab") - 1


def iteration_one(index_ref, slides_ref, step_ref, spatial_ref, temporal_ref, out_weight_ref, embed_ref,
                  states_ref, left_ref, right_ref, *rest):
    frames = states_ref.shape[1]
    has_left, has_right = edge_flags()
    rank = lax.axis_index("tm")

    def latent_of(t, frame):
        if frame < 0:
            return left_ref[t, frame + HALO]
        if frame >= frames:
            return right_ref[t, frame - frames]
        return states_ref[t, frame].astype(BF)

    def valid_of(frame):
        if frame < 0:
            return jnp.where(has_left, 1.0, 0.0)
        if frame >= frames:
            return jnp.where(has_right, 1.0, 0.0)
        return 1.0

    def base_of(frame):
        state = states_ref[0, frame] if 0 <= frame < frames else latent_of(0, frame).astype(F32)
        return jnp.where(rank == 0, state, 0.0)

    one_iteration(0, -1, frames + 1, latent_of, valid_of, base_of,
                  index_ref, slides_ref, step_ref, spatial_ref, temporal_ref, out_weight_ref, embed_ref, *rest)


def iteration_two(index_ref, slides_ref, step_ref, spatial_ref, temporal_ref, out_weight_ref, embed_ref,
                  mine_ref, other_ref, *rest):
    frames = mine_ref.shape[1] - 2
    has_left, has_right = edge_flags()
    rank = lax.axis_index("tm")

    def latent_of(t, frame):
        state = mine_ref[t, frame + 1] + other_ref[t, frame + 1]
        return (state if 0 <= frame < frames else state * valid_of(frame)).astype(BF)

    def valid_of(frame):
        if frame < 0:
            return jnp.where(has_left, 1.0, 0.0)
        if frame >= frames:
            return jnp.where(has_right, 1.0, 0.0)
        return 1.0

    def base_of(frame):
        return jnp.where(rank == 0, mine_ref[0, frame + 1] + other_ref[0, frame + 1], 0.0)

    one_iteration(1, 0, frames, latent_of, valid_of, base_of,
                  index_ref, slides_ref, step_ref, spatial_ref, temporal_ref, out_weight_ref, embed_ref, *rest)


def local(window_states, spatial_weight, temporal_weight, out_weight, time_embed, step_size, time_index, slides):
    times, frames, channels, cells = window_states.shape
    hidden, taps = spatial_weight.shape
    slabs, ranks = lax.axis_size("slab"), lax.axis_size("tm")
    assert ranks == 2 and frames >= HALO
    extra = 16
    rows = ITERS * times
    low, high, embed = pl.pallas_call(
        prepare,
        out_shape=(
            shape((times, HALO, channels, cells), BF),
            shape((times, HALO, channels, cells), BF),
            shape((hidden, rows), F32),
        ),
        in_specs=[SMEM, SMEM, VMEM, ANY],
        out_specs=(VMEM, VMEM, VMEM),
        scratch_shapes=[pltpu.VMEM((rows, hidden), F32), pltpu.SemaphoreType.DMA((rows,))],
        name="prepare",
    )(time_index, slides, window_states, time_embed)
    from_left = lax.ppermute(high, "slab", [(i, i + 1) for i in range(slabs - 1)])
    from_right = lax.ppermute(low, "slab", [(i + 1, i) for i in range(slabs - 1)])

    def iterate(body, name, count, arrays):
        result = shape((times, count, channels, cells), F32)
        return pl.pallas_call(
            body,
            out_shape=(result, result),
            in_specs=[SMEM, SMEM, SMEM] + [VMEM] * (4 + len(arrays)),
            out_specs=(VMEM, VMEM),
            scratch_shapes=[
                pltpu.VMEM((hidden, taps + extra), BF),
                pltpu.VMEM((hidden, 3 * hidden), BF),
                pltpu.VMEM(((count + 2) * hidden, cells), BF),
                pltpu.VMEM((times + 1, count, channels, cells), F32),
            ],
            name=name,
        )(time_index, slides, step_size, spatial_weight, temporal_weight, out_weight, embed, *arrays)

    swap = [(0, 1), (1, 0)]
    mine, sent = iterate(iteration_one, "first_iteration", frames + 2, (window_states, from_left, from_right))
    other = lax.ppermute(sent, "tm", swap)
    mine, sent = iterate(iteration_two, "second_iteration", frames, (mine, other))
    return mine + lax.ppermute(sent, "tm", swap)


def solution(mesh):
    return jax.shard_map(
        local,
        mesh=mesh,
        in_specs=(
            P("tm", ("groups", "slab"), None, None),
            P(), P(), P(), P(), P(),
            P("groups"),
            P("groups"),
        ),
        out_specs=P("tm", ("groups", "slab"), None, None),
        check_vma=False,
    )
```

```python
import jax
import jax.numpy as jnp
from jax import lax
from jax.experimental import pallas as pl
from jax.experimental.pallas import tpu as pltpu
from jax.sharding import PartitionSpec as P

HEIGHT = 16
WIDTH = 32
ITERS = 2
HALO = 2
LANES = 128
EXTRA = 16
BF = jnp.bfloat16
F32 = jnp.float32
MIB = 1 << 20
VMEM = pl.BlockSpec(memory_space=pltpu.VMEM)
SMEM = pl.BlockSpec(memory_space=pltpu.SMEM)
HBM = pl.BlockSpec(memory_space=pltpu.HBM)


def kept(x, space=pltpu.VMEM):
    return pltpu.with_memory_space_constraint(x, space)


def call(body, name, outs, scalars, arrays, scratch, limit):
    return pl.pallas_call(
        body,
        out_shape=tuple(pltpu.VMEM(dims, dtype) for dims, dtype in outs),
        in_specs=[SMEM] * len(scalars) + [VMEM] * len(arrays),
        out_specs=tuple(VMEM for _ in outs),
        scratch_shapes=scratch,
        compiler_params=pltpu.CompilerParams(vmem_limit_bytes=limit * MIB),
        name=name,
    )(*[kept(x, pltpu.SMEM) for x in scalars], *[kept(x) for x in arrays])


def load(states_ref, index_ref, slides_ref, step_ref, *refs):
    count = (len(refs) - 9) // 2
    weights, outs = refs[:count], refs[count : 2 * count]
    states_out, low_ref, high_ref, picks_ref, steps_ref, index_scr, slides_scr, step_scr, sems = refs[2 * count :]
    pairs = [(index_ref, index_scr), (slides_ref, slides_scr), (step_ref, step_scr), (states_ref, states_out)]
    copies = [pltpu.make_async_copy(x, y, sems.at[n]) for n, (x, y) in enumerate(pairs + list(zip(weights, outs)))]
    for copy in copies:
        copy.start()
    for copy in copies[:3]:
        copy.wait()
    times, frames = states_ref.shape[0], states_ref.shape[1]
    first_time = lax.axis_index("tm") * times
    for sweep in range(ITERS):
        offset = first_time if sweep == 0 else first_time + slides_scr[0]
        for i in range(times):
            index = index_scr[offset + i]
            picks_ref[ITERS + sweep * times + i] = index
            steps_ref[sweep * times + i] = step_scr[index]
        picks_ref[sweep] = slides_scr[sweep]
    copies[3].wait()
    low_ref[...] = states_out[:, :HALO].astype(BF)
    high_ref[...] = states_out[:, frames - HALO :].astype(BF)
    for copy in copies[4:]:
        copy.wait()


def silu_half(half):
    return half + half * jnp.tanh(half)


def pack_weights(picks_ref, spatial_ref, temporal_ref, table_ref, spatial_out, temporal_out, last_scr):
    hidden = spatial_out.shape[1]
    taps = spatial_out.shape[2] - EXTRA
    times = spatial_out.shape[0] // ITERS
    steps = table_ref.shape[1]
    full = steps // LANES
    for lag in range(3):
        temporal_out[:, lag * hidden : (lag + 1) * hidden] = (temporal_ref[lag].astype(F32) * 0.5).astype(BF)
    weight = (spatial_ref[...].astype(F32) * 0.5).T.astype(BF)
    if steps % LANES:
        last_scr[:, : steps % LANES] = table_ref[:, full * LANES :]
    lane = lax.broadcasted_iota(jnp.int32, (1, LANES), 1)
    for sweep in range(ITERS):
        for i in range(times):
            index = picks_ref[ITERS + sweep * times + i]
            tile = index // LANES
            start = pl.multiple_of(jnp.minimum(tile, full - 1) * LANES, LANES)
            block = table_ref[:, pl.ds(start, LANES)]
            if steps % LANES:
                block = jnp.where(tile == full, last_scr[...], block)
            place = index - tile * LANES
            whole = pltpu.roll(block, lax.rem(LANES - place, LANES), 1) * 0.5
            rounded = whole.astype(BF).astype(F32)
            rest = pltpu.roll((whole - rounded).astype(BF).astype(F32), 1, 1)
            both = jnp.where(lane == 0, rounded, jnp.where(lane == 1, rest, 0.0))
            slot = sweep * times + i
            spatial_out[slot, :, :taps] = weight
            spatial_out[slot, :, taps:] = both[:, :EXTRA].astype(BF)


def columns_of(latent, valid):
    cells = HEIGHT * WIDTH
    lane = lax.broadcasted_iota(jnp.int32, (1, cells), 1)
    col = lane % WIDTH
    zero = jnp.zeros_like(latent)
    left = jnp.where(col > 0, pltpu.roll(latent, 1, 1), zero)
    right = jnp.where(col < WIDTH - 1, pltpu.roll(latent, cells - 1, 1), zero)
    middle = (left, latent, right)
    above = [jnp.where(lane >= WIDTH, pltpu.roll(x, WIDTH, 1), zero) for x in middle]
    below = [jnp.where(lane < cells - WIDTH, pltpu.roll(x, cells - WIDTH, 1), zero) for x in middle]
    ones = jnp.full((EXTRA, cells), valid, F32).astype(BF)
    return jnp.concatenate([*above, *middle, *below, ones], axis=0)


def stage(sweep, items, latent_of, valid_of, put_first, get_firsts, add_drift, have,
          steps_ref, spatial_ref, temporal_ref, out_weight_ref):
    times = spatial_ref.shape[0] // ITERS
    done = set()

    def convs(t, frame):
        for f in (frame - 1, frame, frame + 1):
            if (t, f) in done or f in have:
                continue
            done.add((t, f))
            half = jnp.dot(spatial_ref[sweep * times + t], columns_of(latent_of(t, f), valid_of(f)),
                           preferred_element_type=F32)
            put_first(t, f, silu_half(half).astype(BF))

    def project(t, frame, second):
        drift = jnp.dot(out_weight_ref[...], second, preferred_element_type=F32)
        add_drift(t, frame, steps_ref[sweep * times + t] * drift)

    waiting = None
    convs(*items[0])
    for n, (t, frame) in enumerate(items):
        if n + 1 < len(items):
            convs(*items[n + 1])
        half = jnp.dot(temporal_ref[...], get_firsts(t, frame), preferred_element_type=F32)
        second = silu_half(half).astype(BF)
        if waiting is not None:
            project(*waiting)
        waiting = (t, frame, second)
    project(*waiting)


def edge_flag(frame, frames):
    slab = lax.axis_index("slab")
    if frame < 0:
        return jnp.where(slab > 0, 1.0, 0.0)
    if frame >= frames:
        return jnp.where(slab < lax.axis_size("slab") - 1, 1.0, 0.0)
    return 1.0


def inner_first(picks_ref, steps_ref, spatial_ref, temporal_ref, table_ref, out_weight_ref, states_ref,
                spatial_out, temporal_out, first_out, sums_out, last_scr):
    times, frames = states_ref.shape[0], states_ref.shape[1]
    hidden = temporal_out.shape[0]
    rank = lax.axis_index("tm")
    pack_weights(picks_ref, spatial_ref, temporal_ref, table_ref, spatial_out, temporal_out, last_scr)
    for frame in range(1, frames - 1):
        sums_out[0, frame - 1] = jnp.where(rank == 0, states_ref[0, frame], 0.0)

    def put_first(t, f, value):
        first_out[t, f * hidden : (f + 1) * hidden, :] = value

    def get_firsts(t, frame):
        return first_out[t, (frame - 1) * hidden : (frame + 2) * hidden, :]

    def add_drift(t, frame, step):
        sums_out[t + 1, frame - 1] = sums_out[t, frame - 1] + step

    stage(0, [(t, f) for t in range(times) for f in range(1, frames - 1)],
          lambda t, f: states_ref[t, f].astype(BF), lambda f: 1.0, put_first, get_firsts, add_drift, (),
          steps_ref, spatial_out, temporal_out, out_weight_ref)


def deliver(slide, times, frame, sums_of, own_ref, send_ref):
    rank = lax.axis_index("tm")
    for j in range(times):
        own_ref[j, frame] = sums_of(jnp.minimum(j + slide, times))
        late = jnp.clip(j + slide - times, 0, times)
        send_ref[j, frame] = sums_of(jnp.where(rank == 0, times, late))


def outer_first(picks_ref, steps_ref, spatial_ref, temporal_ref, out_weight_ref, states_ref,
                left_ref, right_ref, first_ref, inner_ref, own_ref, send_ref, first_scr, sums_scr):
    times, frames = states_ref.shape[0], states_ref.shape[1]
    hidden = temporal_ref.shape[0]
    rank = lax.axis_index("tm")
    outs = [-1, 0, frames - 1, frames]
    halo = [-2, -1, frames, frames + 1]

    def latent_of(t, f):
        return left_ref[t, f + HALO] if f < 0 else right_ref[t, f - frames]

    for n, f in enumerate(outs):
        state = states_ref[0, f] if 0 <= f < frames else latent_of(0, f).astype(F32)
        sums_scr[0, n] = jnp.where(rank == 0, state, 0.0)

    def put_first(t, f, value):
        n = halo.index(f)
        first_scr[t, n * hidden : (n + 1) * hidden, :] = value

    def get_firsts(t, frame):
        parts = []
        for f in (frame - 1, frame, frame + 1):
            if f in halo:
                n = halo.index(f)
                parts.append(first_scr[t, n * hidden : (n + 1) * hidden, :])
            else:
                parts.append(first_ref[t, f * hidden : (f + 1) * hidden, :])
        return jnp.concatenate(parts, axis=0)

    def add_drift(t, frame, step):
        n = outs.index(frame)
        sums_scr[t + 1, n] = sums_scr[t, n] + step

    stage(0, [(t, f) for t in range(times) for f in outs],
          latent_of, lambda f: edge_flag(f, frames), put_first, get_firsts, add_drift, range(frames),
          steps_ref, spatial_ref, temporal_ref, out_weight_ref)
    for f in range(-1, frames + 1):
        sums = (lambda k, n=outs.index(f): sums_scr[k, n]) if f in outs else (lambda k, f=f: inner_ref[k, f - 1])
        deliver(picks_ref[0], times, f + 1, sums, own_ref, send_ref)


def second(picks_ref, steps_ref, spatial_ref, temporal_ref, out_weight_ref, mine_ref, other_ref,
           own_ref, send_ref, first_scr, sums_scr):
    times, frames = own_ref.shape[0], own_ref.shape[1]
    hidden = temporal_ref.shape[0]
    rank = lax.axis_index("tm")

    def state_of(t, f):
        return mine_ref[t, f + 1] + other_ref[t, f + 1]

    def latent_of(t, f):
        state = state_of(t, f)
        return (state if 0 <= f < frames else state * edge_flag(f, frames)).astype(BF)

    for f in range(frames):
        sums_scr[0, f] = jnp.where(rank == 0, state_of(0, f), 0.0)

    def put_first(t, f, value):
        first_scr[t, (f + 1) * hidden : (f + 2) * hidden, :] = value

    def get_firsts(t, frame):
        return first_scr[t, frame * hidden : (frame + 3) * hidden, :]

    def add_drift(t, frame, step):
        sums_scr[t + 1, frame] = sums_scr[t, frame] + step

    stage(1, [(t, f) for t in range(times) for f in range(frames)],
          latent_of, lambda f: edge_flag(f, frames), put_first, get_firsts, add_drift, (),
          steps_ref, spatial_ref, temporal_ref, out_weight_ref)
    for f in range(frames):
        deliver(picks_ref[1], times, f, lambda k, f=f: sums_scr[k, f], own_ref, send_ref)


def local(window_states, spatial_weight, temporal_weight, out_weight, time_embed, step_size, time_index, slides):
    times, frames, channels, cells = window_states.shape
    hidden, taps = spatial_weight.shape
    slabs, ranks = lax.axis_size("slab"), lax.axis_size("tm")
    assert ranks == 2 and frames >= 3 and cells == HEIGHT * WIDTH
    plane = (channels, cells)
    weights = (spatial_weight.T, temporal_weight, time_embed.T, out_weight)
    edge = pltpu.VMEM((times, HALO) + plane, BF)
    *weights, states, low, high, picks, steps = pl.pallas_call(
        load,
        out_shape=(
            *[pltpu.VMEM(x.shape, x.dtype) for x in weights],
            pltpu.VMEM(window_states.shape, F32), edge, edge,
            pltpu.SMEM((ITERS * (times + 1),), jnp.int32), pltpu.SMEM((ITERS * times,), F32),
        ),
        in_specs=[HBM] * (4 + len(weights)),
        out_specs=(*[VMEM] * (3 + len(weights)), SMEM, SMEM),
        scratch_shapes=[
            pltpu.SMEM(time_index.shape, jnp.int32), pltpu.SMEM(slides.shape, jnp.int32),
            pltpu.SMEM(step_size.shape, F32), pltpu.SemaphoreType.DMA((4 + len(weights),)),
        ],
        compiler_params=pltpu.CompilerParams(vmem_limit_bytes=8 * MIB),
        name="load",
    )(*[kept(x, pltpu.HBM) for x in (window_states, time_index, slides, step_size, *weights)])
    spatial, temporal, table, project = weights
    scalars = (picks, steps)
    from_left = lax.ppermute(high, "slab", [(i, i + 1) for i in range(slabs - 1)])
    from_right = lax.ppermute(low, "slab", [(i + 1, i) for i in range(slabs - 1)])
    spatial, temporal, firsts, inner = call(
        inner_first, "inner_first",
        (
            ((ITERS * times, hidden, taps + EXTRA), BF),
            ((hidden, 3 * hidden), BF),
            ((times, frames * hidden, cells), BF),
            ((times + 1, frames - 2) + plane, F32),
        ),
        scalars, (spatial, temporal, table, project, states),
        [pltpu.VMEM((hidden, LANES), F32)], 16,
    )
    wide = ((times, frames + 2) + plane, F32)
    mine, sent = call(
        outer_first, "outer_first", (wide, wide), scalars,
        (spatial, temporal, project, states, from_left, from_right, firsts, inner),
        [pltpu.VMEM((times, 4 * hidden, cells), BF), pltpu.VMEM((times + 1, 4) + plane, F32)], 16,
    )
    swap = [(0, 1), (1, 0)]
    other = lax.ppermute(sent, "tm", swap)
    block = ((times, frames) + plane, F32)
    mine, sent = call(
        second, "second", (block, block), scalars, (spatial, temporal, project, mine, other),
        [pltpu.VMEM((times, (frames + 2) * hidden, cells), BF), pltpu.VMEM((times + 1, frames) + plane, F32)], 24,
    )
    return mine + lax.ppermute(sent, "tm", swap)


def solution(mesh):
    return jax.shard_map(
        local,
        mesh=mesh,
        in_specs=(
            P("tm", ("groups", "slab"), None, None),
            P(), P(), P(), P(), P(),
            P("groups"),
            P("groups"),
        ),
        out_specs=P("tm", ("groups", "slab"), None, None),
        check_vma=False,
    )
```

```python
import jax
import jax.numpy as jnp
from jax import lax
from jax.experimental import pallas as pl
from jax.experimental.pallas import tpu as pltpu
from jax.sharding import PartitionSpec as P

HEIGHT = 16
WIDTH = 32
ITERS = 2
HALO = 2
LANES = 128
EXTRA = 16
BF = jnp.bfloat16
F32 = jnp.float32
MIB = 1 << 20
VMEM = pl.BlockSpec(memory_space=pltpu.VMEM)
SMEM = pl.BlockSpec(memory_space=pltpu.SMEM)
HBM = pl.BlockSpec(memory_space=pltpu.HBM)


def kept(x, space=pltpu.VMEM):
    return pltpu.with_memory_space_constraint(x, space)


def call(body, name, outs, scalars, arrays, scratch, limit):
    return pl.pallas_call(
        body,
        out_shape=tuple(pltpu.VMEM(dims, dtype) for dims, dtype in outs),
        in_specs=[SMEM] * len(scalars) + [VMEM] * len(arrays),
        out_specs=tuple(VMEM for _ in outs),
        scratch_shapes=scratch,
        compiler_params=pltpu.CompilerParams(vmem_limit_bytes=limit * MIB),
        name=name,
    )(*[kept(x, pltpu.SMEM) for x in scalars], *[kept(x) for x in arrays])


def load(states_ref, index_ref, slides_ref, step_ref, *refs):
    count = (len(refs) - 9) // 2
    weights, outs = refs[:count], refs[count : 2 * count]
    states_out, low_ref, high_ref, picks_ref, steps_ref, index_scr, slides_scr, step_scr, sems = refs[2 * count :]
    pairs = [(index_ref, index_scr), (slides_ref, slides_scr), (step_ref, step_scr), (states_ref, states_out)]
    copies = [pltpu.make_async_copy(x, y, sems.at[n]) for n, (x, y) in enumerate(pairs + list(zip(weights, outs)))]
    for copy in copies:
        copy.start()
    for copy in copies[:3]:
        copy.wait()
    times, frames = states_ref.shape[0], states_ref.shape[1]
    first_time = lax.axis_index("tm") * times
    for sweep in range(ITERS):
        offset = first_time if sweep == 0 else first_time + slides_scr[0]
        for i in range(times):
            index = index_scr[offset + i]
            picks_ref[ITERS + sweep * times + i] = index
            steps_ref[sweep * times + i] = step_scr[index]
        picks_ref[sweep] = slides_scr[sweep]
    copies[3].wait()
    for ref, first in ((low_ref, 0), (high_ref, frames - HALO)):
        edge = states_out[:, first : first + HALO]
        rounded = edge.astype(BF)
        ref[:times] = rounded
        ref[times] = (edge[0] - rounded[0].astype(F32)).astype(BF)
    for copy in copies[4:]:
        copy.wait()


def silu_half(half):
    return half + half * jnp.tanh(half)


def pack_weights(picks_ref, spatial_ref, temporal_ref, table_ref, spatial_out, temporal_out, last_scr):
    hidden = spatial_out.shape[0]
    taps = spatial_out.shape[1] - EXTRA
    slots = EXTRA // 2
    steps = table_ref.shape[1]
    full = steps // LANES
    if steps % LANES:
        last_scr[:, : steps % LANES] = table_ref[:, full * LANES :]
    lane = lax.broadcasted_iota(jnp.int32, (1, LANES), 1)
    inset = taps % LANES
    embed = jnp.zeros((hidden, LANES), F32)
    for slot in range(slots):
        index = picks_ref[ITERS + slot]
        tile = index // LANES
        start = pl.multiple_of(jnp.minimum(tile, full - 1) * LANES, LANES)
        block = table_ref[:, pl.ds(start, LANES)]
        if steps % LANES:
            block = jnp.where(tile == full, last_scr[...], block)
        place = index - tile * LANES
        shift = lax.rem(inset + slot + LANES - place, LANES)
        embed = jnp.where(lane == inset + slot, pltpu.roll(block, shift, 1), embed)
    embed = embed * 0.5
    rounded = embed.astype(BF).astype(F32)
    extra = rounded + pltpu.roll(embed - rounded, slots, 1)
    weight = (spatial_ref[...].astype(F32) * 0.5).T.astype(BF)
    spatial_out[:, : taps - inset] = weight[:, : taps - inset]
    spatial_out[:, taps - inset :] = extra[:, : inset + EXTRA].astype(BF)
    spatial_out[:, taps - inset : taps] = weight[:, taps - inset :]
    for lag in range(3):
        temporal_out[:, lag * hidden : (lag + 1) * hidden] = temporal_ref[lag] * 0.5


def columns_of(latent, valid, slot):
    cells = HEIGHT * WIDTH
    lane = lax.broadcasted_iota(jnp.int32, (1, cells), 1)
    col = lane % WIDTH
    zero = jnp.zeros_like(latent)
    left = jnp.where(col > 0, pltpu.roll(latent, 1, 1), zero)
    right = jnp.where(col < WIDTH - 1, pltpu.roll(latent, cells - 1, 1), zero)
    middle = (left, latent, right)
    above = [jnp.where(lane >= WIDTH, pltpu.roll(x, WIDTH, 1), zero) for x in middle]
    below = [jnp.where(lane < cells - WIDTH, pltpu.roll(x, cells - WIDTH, 1), zero) for x in middle]
    row = lax.broadcasted_iota(jnp.int32, (EXTRA, cells), 0)
    picks = jnp.where(lax.rem(row, EXTRA // 2) == slot, valid, 0.0).astype(BF)
    return jnp.concatenate([*above, *middle, *below, picks], axis=0)


def stage(sweep, items, latent_of, valid_of, put_first, get_firsts, add_drift, have,
          steps_ref, spatial_ref, temporal_ref, out_weight_ref):
    times = EXTRA // 2 // ITERS
    done = set()

    def convs(t, frame):
        for f in (frame - 1, frame, frame + 1):
            if (t, f) in done or f in have:
                continue
            done.add((t, f))
            columns = columns_of(latent_of(t, f), valid_of(f), sweep * times + t)
            half = jnp.dot(spatial_ref[...], columns, preferred_element_type=F32)
            put_first(t, f, silu_half(half).astype(BF))

    def project(t, frame, second):
        drift = jnp.dot(out_weight_ref[...], second, preferred_element_type=F32)
        add_drift(t, frame, steps_ref[sweep * times + t] * drift)

    waiting = None
    convs(*items[0])
    for n, (t, frame) in enumerate(items):
        if n + 1 < len(items):
            convs(*items[n + 1])
        half = jnp.dot(temporal_ref[...], get_firsts(t, frame), preferred_element_type=F32)
        second = silu_half(half).astype(BF)
        if waiting is not None:
            project(*waiting)
        waiting = (t, frame, second)
    project(*waiting)


def edge_flag(frame, frames):
    slab = lax.axis_index("slab")
    if frame < 0:
        return jnp.where(slab > 0, 1.0, 0.0)
    if frame >= frames:
        return jnp.where(slab < lax.axis_size("slab") - 1, 1.0, 0.0)
    return 1.0


def inner_first(picks_ref, steps_ref, spatial_ref, temporal_ref, table_ref, out_weight_ref, states_ref,
                spatial_out, temporal_out, first_out, sums_out, last_scr):
    times, frames = states_ref.shape[0], states_ref.shape[1]
    hidden = temporal_out.shape[0]
    rank = lax.axis_index("tm")
    pack_weights(picks_ref, spatial_ref, temporal_ref, table_ref, spatial_out, temporal_out, last_scr)
    for frame in range(1, frames - 1):
        sums_out[0, frame - 1] = jnp.where(rank == 0, states_ref[0, frame], 0.0)

    def put_first(t, f, value):
        first_out[t, f * hidden : (f + 1) * hidden, :] = value

    def get_firsts(t, frame):
        return first_out[t, (frame - 1) * hidden : (frame + 2) * hidden, :]

    def add_drift(t, frame, step):
        sums_out[t + 1, frame - 1] = sums_out[t, frame - 1] + step

    stage(0, [(t, f) for t in range(times) for f in range(1, frames - 1)],
          lambda t, f: states_ref[t, f].astype(BF), lambda f: 1.0, put_first, get_firsts, add_drift, (),
          steps_ref, spatial_out, temporal_out, out_weight_ref)


def deliver(slide, times, frame, sums_of, own_ref, send_ref):
    rank = lax.axis_index("tm")
    for j in range(times):
        own_ref[j, frame] = sums_of(jnp.minimum(j + slide, times))
        late = jnp.clip(j + slide - times, 0, times)
        sent = sums_of(jnp.where(rank == 0, times, late))
        send_ref[j, frame] = sent.astype(send_ref.dtype)
        if send_ref.shape[0] > times and j == 0:
            send_ref[times, frame] = (sent - sent.astype(BF).astype(F32)).astype(BF)


def outer_first(picks_ref, steps_ref, spatial_ref, temporal_ref, out_weight_ref, states_ref,
                left_ref, right_ref, first_ref, inner_ref, own_ref, send_ref, first_scr, sums_scr):
    times, frames = states_ref.shape[0], states_ref.shape[1]
    hidden = temporal_ref.shape[0]
    rank = lax.axis_index("tm")
    outs = [-1, 0, frames - 1, frames]
    halo = [-2, -1, frames, frames + 1]

    def latent_of(t, f):
        return left_ref[t, f + HALO] if f < 0 else right_ref[t, f - frames]

    for n, f in enumerate(outs):
        if 0 <= f < frames:
            state = states_ref[0, f]
        else:
            state = latent_of(0, f).astype(F32) + latent_of(times, f).astype(F32)
        sums_scr[0, n] = jnp.where(rank == 0, state, 0.0)

    def put_first(t, f, value):
        n = halo.index(f)
        first_scr[t, n * hidden : (n + 1) * hidden, :] = value

    def get_firsts(t, frame):
        parts = []
        for f in (frame - 1, frame, frame + 1):
            if f in halo:
                n = halo.index(f)
                parts.append(first_scr[t, n * hidden : (n + 1) * hidden, :])
            else:
                parts.append(first_ref[t, f * hidden : (f + 1) * hidden, :])
        return jnp.concatenate(parts, axis=0)

    def add_drift(t, frame, step):
        n = outs.index(frame)
        sums_scr[t + 1, n] = sums_scr[t, n] + step

    stage(0, [(t, f) for t in range(times) for f in outs],
          latent_of, lambda f: edge_flag(f, frames), put_first, get_firsts, add_drift, range(frames),
          steps_ref, spatial_ref, temporal_ref, out_weight_ref)
    for f in range(-1, frames + 1):
        sums = (lambda k, n=outs.index(f): sums_scr[k, n]) if f in outs else (lambda k, f=f: inner_ref[k, f - 1])
        deliver(picks_ref[0], times, f + 1, sums, own_ref, send_ref)


def second(picks_ref, steps_ref, spatial_ref, temporal_ref, out_weight_ref, mine_ref, other_ref,
           own_ref, send_ref, first_scr, sums_scr):
    times, frames = own_ref.shape[0], own_ref.shape[1]
    hidden = temporal_ref.shape[0]
    rank = lax.axis_index("tm")

    def state_of(t, f):
        rest = other_ref[times, f + 1].astype(F32)
        if t > 0:
            rest = rest * jnp.where(rank == 0, 0.0, 1.0)
        return mine_ref[t, f + 1] + (other_ref[t, f + 1].astype(F32) + rest)

    def latent_of(t, f):
        state = state_of(t, f)
        return (state if 0 <= f < frames else state * edge_flag(f, frames)).astype(BF)

    for f in range(frames):
        sums_scr[0, f] = jnp.where(rank == 0, state_of(0, f), 0.0)

    def put_first(t, f, value):
        first_scr[t, (f + 1) * hidden : (f + 2) * hidden, :] = value

    def get_firsts(t, frame):
        return first_scr[t, frame * hidden : (frame + 3) * hidden, :]

    def add_drift(t, frame, step):
        sums_scr[t + 1, frame] = sums_scr[t, frame] + step

    stage(1, [(t, f) for t in range(times) for f in range(frames)],
          latent_of, lambda f: edge_flag(f, frames), put_first, get_firsts, add_drift, (),
          steps_ref, spatial_ref, temporal_ref, out_weight_ref)
    for f in range(frames):
        deliver(picks_ref[1], times, f, lambda k, f=f: sums_scr[k, f], own_ref, send_ref)


def local(window_states, spatial_weight, temporal_weight, out_weight, time_embed, step_size, time_index, slides):
    times, frames, channels, cells = window_states.shape
    hidden, taps = spatial_weight.shape
    slabs, ranks = lax.axis_size("slab"), lax.axis_size("tm")
    assert ranks == 2 and EXTRA == 2 * ITERS * times and frames >= 3 and cells == HEIGHT * WIDTH
    plane = (channels, cells)
    weights = (spatial_weight.T, temporal_weight, time_embed.T, out_weight)
    edge = pltpu.VMEM((times + 1, HALO) + plane, BF)
    *weights, states, low, high, picks, steps = pl.pallas_call(
        load,
        out_shape=(
            *[pltpu.VMEM(x.shape, x.dtype) for x in weights],
            pltpu.VMEM(window_states.shape, F32), edge, edge,
            pltpu.SMEM((ITERS * (times + 1),), jnp.int32), pltpu.SMEM((ITERS * times,), F32),
        ),
        in_specs=[HBM] * (4 + len(weights)),
        out_specs=(*[VMEM] * (3 + len(weights)), SMEM, SMEM),
        scratch_shapes=[
            pltpu.SMEM(time_index.shape, jnp.int32), pltpu.SMEM(slides.shape, jnp.int32),
            pltpu.SMEM(step_size.shape, F32), pltpu.SemaphoreType.DMA((4 + len(weights),)),
        ],
        compiler_params=pltpu.CompilerParams(vmem_limit_bytes=8 * MIB),
        name="load",
    )(*[kept(x, pltpu.HBM) for x in (window_states, time_index, slides, step_size, *weights)])
    spatial, temporal, table, project = weights
    scalars = (picks, steps)
    from_left = lax.ppermute(high, "slab", [(i, i + 1) for i in range(slabs - 1)])
    from_right = lax.ppermute(low, "slab", [(i + 1, i) for i in range(slabs - 1)])
    spatial, temporal, firsts, inner = call(
        inner_first, "inner_first",
        (
            ((hidden, taps + EXTRA), BF),
            ((hidden, 3 * hidden), BF),
            ((times, frames * hidden, cells), BF),
            ((times + 1, frames - 2) + plane, F32),
        ),
        scalars, (spatial, temporal, table, project, states),
        [pltpu.VMEM((hidden, LANES), F32)], 16,
    )
    wide = ((times, frames + 2) + plane, F32)
    mine, sent = call(
        outer_first, "outer_first", (wide, ((times + 1, frames + 2) + plane, BF)), scalars,
        (spatial, temporal, project, states, from_left, from_right, firsts, inner),
        [pltpu.VMEM((times, 4 * hidden, cells), BF), pltpu.VMEM((times + 1, 4) + plane, F32)], 16,
    )
    swap = [(0, 1), (1, 0)]
    other = lax.ppermute(sent, "tm", swap)
    block = ((times, frames) + plane, F32)
    mine, sent = call(
        second, "second", (block, block), scalars, (spatial, temporal, project, mine, other),
        [pltpu.VMEM((times, (frames + 2) * hidden, cells), BF), pltpu.VMEM((times + 1, frames) + plane, F32)], 24,
    )
    return mine + lax.ppermute(sent, "tm", swap)


def solution(mesh):
    return jax.shard_map(
        local,
        mesh=mesh,
        in_specs=(
            P("tm", ("groups", "slab"), None, None),
            P(), P(), P(), P(), P(),
            P("groups"),
            P("groups"),
        ),
        out_specs=P("tm", ("groups", "slab"), None, None),
        check_vma=False,
    )
```

```python
import jax
import jax.numpy as jnp
from jax import lax
from jax.experimental import pallas as pl
from jax.experimental.pallas import tpu as pltpu
from jax.sharding import PartitionSpec as P

HEIGHT = 16
WIDTH = 32
ITERS = 2
HALO = 2
LANES = 128
EXTRA = 16
BF = jnp.bfloat16
F32 = jnp.float32
MIB = 1 << 20
TILE = 256
PIECE = 64
VMEM = pl.BlockSpec(memory_space=pltpu.VMEM)
SMEM = pl.BlockSpec(memory_space=pltpu.SMEM)
HBM = pl.BlockSpec(memory_space=pltpu.HBM)


def kept(x, space=pltpu.VMEM):
    return pltpu.with_memory_space_constraint(x, space)


def call(body, name, outs, scalars, arrays, scratch, limit):
    return pl.pallas_call(
        body,
        out_shape=tuple(pltpu.VMEM(dims, dtype) for dims, dtype in outs),
        in_specs=[SMEM] * len(scalars) + [VMEM] * len(arrays),
        out_specs=tuple(VMEM for _ in outs),
        scratch_shapes=scratch,
        compiler_params=pltpu.CompilerParams(vmem_limit_bytes=limit * MIB),
        name=name,
    )(*[kept(x, pltpu.SMEM) for x in scalars], *[kept(x) for x in arrays])


def load(states_ref, index_ref, slides_ref, step_ref, *refs):
    count = (len(refs) - 9) // 2
    weights, outs = refs[:count], refs[count : 2 * count]
    states_out, low_ref, high_ref, picks_ref, steps_ref, index_scr, slides_scr, step_scr, sems = refs[2 * count :]
    pairs = [(index_ref, index_scr), (slides_ref, slides_scr), (step_ref, step_scr), (states_ref, states_out)]
    copies = [pltpu.make_async_copy(x, y, sems.at[n]) for n, (x, y) in enumerate(pairs + list(zip(weights, outs)))]
    for copy in copies:
        copy.start()
    for copy in copies[:3]:
        copy.wait()
    times, frames = states_ref.shape[0], states_ref.shape[1]
    first_time = lax.axis_index("tm") * times
    for sweep in range(ITERS):
        offset = first_time if sweep == 0 else first_time + slides_scr[0]
        for i in range(times):
            index = index_scr[offset + i]
            picks_ref[ITERS + sweep * times + i] = index
            steps_ref[sweep * times + i] = step_scr[index]
        picks_ref[sweep] = slides_scr[sweep]
    copies[3].wait()
    for ref, first in ((low_ref, 0), (high_ref, frames - HALO)):
        edge = states_out[:, first : first + HALO]
        rounded = edge.astype(BF)
        ref[:times] = rounded
        ref[times] = (edge[0] - rounded[0].astype(F32)).astype(BF)
    for copy in copies[4:]:
        copy.wait()


def silu_half(half):
    return half + half * jnp.tanh(half)


def pack_weights(picks_ref, spatial_ref, temporal_ref, table_ref, spatial_out, temporal_out, project_ref, project_out, last_scr):
    hidden = spatial_out.shape[0]
    taps = spatial_ref.shape[0]
    slots = EXTRA // 2
    steps = table_ref.shape[1]
    full = steps // LANES
    if steps % LANES:
        last_scr[:, : steps % LANES] = table_ref[:, full * LANES :]
    lane = lax.broadcasted_iota(jnp.int32, (1, LANES), 1)
    inset = taps % LANES
    embed = jnp.zeros((hidden, LANES), F32)
    for slot in range(slots):
        index = picks_ref[ITERS + slot]
        tile = index // LANES
        start = pl.multiple_of(jnp.minimum(tile, full - 1) * LANES, LANES)
        block = table_ref[:, pl.ds(start, LANES)]
        if steps % LANES:
            block = jnp.where(tile == full, last_scr[...], block)
        place = index - tile * LANES
        shift = lax.rem(inset + slot + LANES - place, LANES)
        embed = jnp.where(lane == inset + slot, pltpu.roll(block, shift, 1), embed)
    embed = embed * 0.5
    rounded = embed.astype(BF).astype(F32)
    extra = rounded + pltpu.roll(embed - rounded, slots, 1)
    weight = (spatial_ref[...].astype(F32) * 0.5).T.astype(BF)
    spatial_out[:, : taps - inset] = weight[:, : taps - inset]
    spatial_out[:, taps - inset :] = extra.astype(BF)
    spatial_out[:, taps - inset : taps] = weight[:, taps - inset :]
    for lag in range(3):
        temporal_out[:, lag * hidden : (lag + 1) * hidden] = temporal_ref[lag] * 0.5
    for ref, used in ((temporal_out, 3 * hidden), (project_out, hidden)):
        if used < ref.shape[1]:
            ref[:, used:] = jnp.zeros((ref.shape[0], ref.shape[1] - used), BF)
    project_out[:, :hidden] = project_ref[...]


def columns_of(latent, valid, slot):
    cells = HEIGHT * WIDTH
    lane = lax.broadcasted_iota(jnp.int32, (1, cells), 1)
    col = lane % WIDTH
    zero = jnp.zeros_like(latent)
    left = jnp.where(col > 0, pltpu.roll(latent, 1, 1), zero)
    right = jnp.where(col < WIDTH - 1, pltpu.roll(latent, cells - 1, 1), zero)
    middle = (left, latent, right)
    above = [jnp.where(lane >= WIDTH, pltpu.roll(x, WIDTH, 1), zero) for x in middle]
    below = [jnp.where(lane < cells - WIDTH, pltpu.roll(x, cells - WIDTH, 1), zero) for x in middle]
    row = lax.broadcasted_iota(jnp.int32, (EXTRA, cells), 0)
    picks = jnp.where(lax.rem(row, EXTRA // 2) == slot, valid, 0.0).astype(BF)
    return jnp.concatenate([*above, *middle, *below, picks], axis=0)


def filled(parts, width):
    rows = sum(x.shape[0] for x in parts)
    if rows < TILE:
        parts = [*parts, jnp.zeros((TILE - rows, width), BF)]
    return parts[0] if len(parts) == 1 else jnp.concatenate(parts, axis=0)


def stage(sweep, items, latent_of, valid_of, put_first, first_at, add_drift, have,
          steps_ref, spatial_ref, temporal_ref, project_ref):
    times = EXTRA // 2 // ITERS
    hidden = spatial_ref.shape[0]
    pieces = hidden // PIECE
    units = range(2)
    halves = [slice(q * TILE, (q + 1) * TILE) for q in units]
    order, needed = [], []
    for t, frame in items:
        for f in (frame - 1, frame, frame + 1):
            if (t, f) not in order and f not in have:
                order.append((t, f))
        needed.append(len(order))
    last = len(items) - 1

    def run(*accs):
        per = 3 * pieces + 1
        sets = [[[accs[q * per + k * pieces + i] for i in range(pieces)] for q in units] for k in range(3)]
        small = [accs[q * per + 3 * pieces] for q in units]
        state = {"pass": 0, "issued": 0}

        def one_pass(tiles, outs, lhs_of):
            register = state["pass"] % 2
            state["pass"] += 1
            for q in units:
                pltpu.matmul_push_rhs(tiles[q], staging_register=register, mxu_index=q)
            for i in range(len(outs[0])):
                lhs = lhs_of(i)
                for q in units:
                    pltpu.matmul_acc_lhs(outs[q][i], lhs, load_staged_rhs=register if i == 0 else None)

        def conv(into):
            t, f = order[state["issued"]]
            state["issued"] += 1
            columns = columns_of(latent_of(t, f), valid_of(f), sweep * times + t)
            tiles = [filled([columns[:, h]], TILE) for h in halves]
            one_pass(tiles, sets[into], lambda i: spatial_ref[i * PIECE : (i + 1) * PIECE, :])
            return t, f, into

        def finish_conv(t, f, into):
            for i in range(pieces):
                for q in units:
                    value = silu_half(pltpu.matmul_pop(sets[into][q][i])).astype(BF)
                    put_first(t, f, value, i * PIECE, halves[q])

        def temporal(n, k):
            t, frame = items[n]
            low, high = k * TILE, min((k + 1) * TILE, 3 * hidden)
            tiles = []
            for h in halves:
                parts = []
                for d in range(3):
                    start, stop = max(low, d * hidden), min(high, (d + 1) * hidden)
                    if start < stop:
                        parts.append(first_at(t, frame - 1 + d, start - d * hidden, stop - d * hidden, h))
                tiles.append(filled(parts, TILE))
            one_pass(tiles, sets[n % 2], lambda i: temporal_ref[i * PIECE : (i + 1) * PIECE, low : low + TILE])

        def finish_temporal(n):
            return [[silu_half(pltpu.matmul_pop(sets[n % 2][q][i])).astype(BF) for i in range(pieces)] for q in units]

        def project(second, k):
            count = TILE // PIECE
            tiles = [filled(second[q][k * count : (k + 1) * count], TILE) for q in units]
            one_pass(tiles, [[x] for x in small], lambda i: project_ref[:, k * TILE : (k + 1) * TILE])

        def finish_project(n):
            t, frame = items[n]
            for q in units:
                add_drift(t, frame, steps_ref[sweep * times + t] * pltpu.matmul_pop(small[q]), halves[q])

        temporal_passes = pl.cdiv(3 * hidden, TILE)
        project_passes = pl.cdiv(hidden, TILE)
        assert temporal_passes == 4 and project_passes == 2
        pending = None
        for i in range(needed[0]):
            issued = conv(2 if (needed[0] - 1 - i) % 2 == 0 else 1)
            if pending is not None:
                finish_conv(*pending)
            pending = issued
        second = None
        for n in range(len(items)):
            ahead = needed[min(n + 2, last)]
            temporal(n, 0)
            if pending is not None:
                finish_conv(*pending)
                pending = None
            early = conv(2) if state["issued"] < ahead else None
            temporal(n, 1)
            if n > 0:
                second = finish_temporal(n - 1)
            if n > 1:
                finish_project(n - 2)
            temporal(n, 2)
            if n > 0:
                project(second, 0)
            if early is not None:
                finish_conv(*early)
            pending = conv(2) if state["issued"] < ahead else None
            temporal(n, 3)
            if n > 0:
                project(second, 1)
            assert n == last or state["issued"] >= needed[n + 1]
        second = finish_temporal(last)
        if last > 0:
            finish_project(last - 1)
        project(second, 0)
        project(second, 1)
        finish_project(last)

    shapes = [(PIECE, TILE)] * (3 * pieces) + [(project_ref.shape[0], TILE)]
    pl.run_scoped(run, *[pltpu.ACC(q)(dims, F32) for q in units for dims in shapes])


def edge_flag(frame, frames):
    slab = lax.axis_index("slab")
    if frame < 0:
        return jnp.where(slab > 0, 1.0, 0.0)
    if frame >= frames:
        return jnp.where(slab < lax.axis_size("slab") - 1, 1.0, 0.0)
    return 1.0


def inner_first(picks_ref, steps_ref, spatial_ref, temporal_ref, table_ref, out_weight_ref, states_ref,
                spatial_out, temporal_out, project_out, first_out, sums_out, last_scr):
    times, frames = states_ref.shape[0], states_ref.shape[1]
    hidden = temporal_out.shape[0]
    rank = lax.axis_index("tm")
    pack_weights(picks_ref, spatial_ref, temporal_ref, table_ref, spatial_out, temporal_out, out_weight_ref, project_out, last_scr)
    for frame in range(1, frames - 1):
        sums_out[0, frame - 1] = jnp.where(rank == 0, states_ref[0, frame], 0.0)

    def put_first(t, f, value, row, half):
        first_out[t, f * hidden + row : f * hidden + row + PIECE, half] = value

    def first_at(t, f, start, stop, half):
        return first_out[t, f * hidden + start : f * hidden + stop, half]

    def add_drift(t, frame, step, half):
        sums_out[t + 1, frame - 1, :, half] = sums_out[t, frame - 1, :, half] + step

    stage(0, [(t, f) for t in range(times) for f in range(1, frames - 1)],
          lambda t, f: states_ref[t, f].astype(BF), lambda f: 1.0, put_first, first_at, add_drift, (),
          steps_ref, spatial_out, temporal_out, project_out)


def deliver(slide, times, frame, sums_of, own_ref, send_ref):
    rank = lax.axis_index("tm")
    for j in range(times):
        own_ref[j, frame] = sums_of(jnp.minimum(j + slide, times))
        late = jnp.clip(j + slide - times, 0, times)
        sent = sums_of(jnp.where(rank == 0, times, late))
        send_ref[j, frame] = sent.astype(send_ref.dtype)
        if send_ref.shape[0] > times and j == 0:
            send_ref[times, frame] = (sent - sent.astype(BF).astype(F32)).astype(BF)


def outer_first(picks_ref, steps_ref, spatial_ref, temporal_ref, out_weight_ref, states_ref,
                left_ref, right_ref, first_ref, inner_ref, own_ref, send_ref, first_scr, sums_scr):
    times, frames = states_ref.shape[0], states_ref.shape[1]
    hidden = temporal_ref.shape[0]
    rank = lax.axis_index("tm")
    outs = [-1, 0, frames - 1, frames]
    halo = [-2, -1, frames, frames + 1]

    def latent_of(t, f):
        return left_ref[t, f + HALO] if f < 0 else right_ref[t, f - frames]

    for n, f in enumerate(outs):
        if 0 <= f < frames:
            state = states_ref[0, f]
        else:
            state = latent_of(0, f).astype(F32) + latent_of(times, f).astype(F32)
        sums_scr[0, n] = jnp.where(rank == 0, state, 0.0)

    def put_first(t, f, value, row, half):
        start = halo.index(f) * hidden + row
        first_scr[t, start : start + PIECE, half] = value

    def first_at(t, f, start, stop, half):
        if f in halo:
            n = halo.index(f)
            return first_scr[t, n * hidden + start : n * hidden + stop, half]
        return first_ref[t, f * hidden + start : f * hidden + stop, half]

    def add_drift(t, frame, step, half):
        n = outs.index(frame)
        sums_scr[t + 1, n, :, half] = sums_scr[t, n, :, half] + step

    stage(0, [(t, f) for t in range(times) for f in outs],
          latent_of, lambda f: edge_flag(f, frames), put_first, first_at, add_drift, range(frames),
          steps_ref, spatial_ref, temporal_ref, out_weight_ref)
    for f in range(-1, frames + 1):
        sums = (lambda k, n=outs.index(f): sums_scr[k, n]) if f in outs else (lambda k, f=f: inner_ref[k, f - 1])
        deliver(picks_ref[0], times, f + 1, sums, own_ref, send_ref)


def second(picks_ref, steps_ref, spatial_ref, temporal_ref, out_weight_ref, mine_ref, other_ref,
           own_ref, send_ref, first_scr, sums_scr):
    times, frames = own_ref.shape[0], own_ref.shape[1]
    hidden = temporal_ref.shape[0]
    rank = lax.axis_index("tm")

    def state_of(t, f):
        rest = other_ref[times, f + 1].astype(F32)
        if t > 0:
            rest = rest * jnp.where(rank == 0, 0.0, 1.0)
        return mine_ref[t, f + 1] + (other_ref[t, f + 1].astype(F32) + rest)

    def latent_of(t, f):
        state = state_of(t, f)
        return (state if 0 <= f < frames else state * edge_flag(f, frames)).astype(BF)

    for f in range(frames):
        sums_scr[0, f] = jnp.where(rank == 0, state_of(0, f), 0.0)

    def put_first(t, f, value, row, half):
        start = (f + 1) * hidden + row
        first_scr[t, start : start + PIECE, half] = value

    def first_at(t, f, start, stop, half):
        return first_scr[t, (f + 1) * hidden + start : (f + 1) * hidden + stop, half]

    def add_drift(t, frame, step, half):
        sums_scr[t + 1, frame, :, half] = sums_scr[t, frame, :, half] + step

    stage(1, [(t, f) for t in range(times) for f in range(frames)],
          latent_of, lambda f: edge_flag(f, frames), put_first, first_at, add_drift, (),
          steps_ref, spatial_ref, temporal_ref, out_weight_ref)
    for f in range(frames):
        deliver(picks_ref[1], times, f, lambda k, f=f: sums_scr[k, f], own_ref, send_ref)


def local(window_states, spatial_weight, temporal_weight, out_weight, time_embed, step_size, time_index, slides):
    times, frames, channels, cells = window_states.shape
    hidden, taps = spatial_weight.shape
    slabs, ranks = lax.axis_size("slab"), lax.axis_size("tm")
    assert ranks == 2 and EXTRA == 2 * ITERS * times and hidden % PIECE == 0
    assert taps - taps % LANES + LANES == TILE and frames >= 3 and cells == HEIGHT * WIDTH
    plane = (channels, cells)
    weights = (spatial_weight.T, temporal_weight, time_embed.T, out_weight)
    edge = pltpu.VMEM((times + 1, HALO) + plane, BF)
    *weights, states, low, high, picks, steps = pl.pallas_call(
        load,
        out_shape=(
            *[pltpu.VMEM(x.shape, x.dtype) for x in weights],
            pltpu.VMEM(window_states.shape, F32), edge, edge,
            pltpu.SMEM((ITERS * (times + 1),), jnp.int32), pltpu.SMEM((ITERS * times,), F32),
        ),
        in_specs=[HBM] * (4 + len(weights)),
        out_specs=(*[VMEM] * (3 + len(weights)), SMEM, SMEM),
        scratch_shapes=[
            pltpu.SMEM(time_index.shape, jnp.int32), pltpu.SMEM(slides.shape, jnp.int32),
            pltpu.SMEM(step_size.shape, F32), pltpu.SemaphoreType.DMA((4 + len(weights),)),
        ],
        compiler_params=pltpu.CompilerParams(vmem_limit_bytes=8 * MIB),
        name="load",
    )(*[kept(x, pltpu.HBM) for x in (window_states, time_index, slides, step_size, *weights)])
    spatial, temporal, table, project = weights
    scalars = (picks, steps)
    from_left = lax.ppermute(high, "slab", [(i, i + 1) for i in range(slabs - 1)])
    from_right = lax.ppermute(low, "slab", [(i + 1, i) for i in range(slabs - 1)])
    spatial, temporal, project, firsts, inner = call(
        inner_first, "inner_first",
        (
            ((hidden, TILE), BF),
            ((hidden, pl.cdiv(3 * hidden, TILE) * TILE), BF),
            ((channels, pl.cdiv(hidden, TILE) * TILE), BF),
            ((times, frames * hidden, cells), BF),
            ((times + 1, frames - 2) + plane, F32),
        ),
        scalars, (spatial, temporal, table, project, states),
        [pltpu.VMEM((hidden, LANES), F32)], 16,
    )
    wide = ((times, frames + 2) + plane, F32)
    mine, sent = call(
        outer_first, "outer_first", (wide, ((times + 1, frames + 2) + plane, BF)), scalars,
        (spatial, temporal, project, states, from_left, from_right, firsts, inner),
        [pltpu.VMEM((times, 4 * hidden, cells), BF), pltpu.VMEM((times + 1, 4) + plane, F32)], 16,
    )
    swap = [(0, 1), (1, 0)]
    other = lax.ppermute(sent, "tm", swap)
    block = ((times, frames) + plane, F32)
    mine, sent = call(
        second, "second", (block, block), scalars, (spatial, temporal, project, mine, other),
        [pltpu.VMEM((times, (frames + 2) * hidden, cells), BF), pltpu.VMEM((times + 1, frames) + plane, F32)], 24,
    )
    return mine + lax.ppermute(sent, "tm", swap)


def solution(mesh):
    return jax.shard_map(
        local,
        mesh=mesh,
        in_specs=(
            P("tm", ("groups", "slab"), None, None),
            P(), P(), P(), P(), P(),
            P("groups"),
            P("groups"),
        ),
        out_specs=P("tm", ("groups", "slab"), None, None),
        check_vma=False,
    )
```

```python
import jax
import jax.numpy as jnp
from jax import lax
from jax.experimental import pallas as pl
from jax.experimental.pallas import tpu as pltpu
from jax.sharding import PartitionSpec as P

HEIGHT = 16
WIDTH = 32
ITERS = 2
HALO = 2
LANES = 128
EXTRA = 16
BF = jnp.bfloat16
F32 = jnp.float32
MIB = 1 << 20
TILE = 256
PIECE = 64
VMEM = pl.BlockSpec(memory_space=pltpu.VMEM)
SMEM = pl.BlockSpec(memory_space=pltpu.SMEM)
HBM = pl.BlockSpec(memory_space=pltpu.HBM)


def kept(x, space=pltpu.VMEM):
    return pltpu.with_memory_space_constraint(x, space)


def call(body, name, outs, scalars, arrays, scratch, limit):
    return pl.pallas_call(
        body,
        out_shape=tuple(pltpu.VMEM(dims, dtype) for dims, dtype in outs),
        in_specs=[SMEM] * len(scalars) + [VMEM] * len(arrays),
        out_specs=tuple(VMEM for _ in outs),
        scratch_shapes=scratch,
        compiler_params=pltpu.CompilerParams(vmem_limit_bytes=limit * MIB),
        name=name,
    )(*[kept(x, pltpu.SMEM) for x in scalars], *[kept(x) for x in arrays])


def load(states_ref, index_ref, slides_ref, step_ref, *refs):
    count = (len(refs) - 9) // 2
    weights, outs = refs[:count], refs[count : 2 * count]
    states_out, low_ref, high_ref, picks_ref, steps_ref, index_scr, slides_scr, step_scr, sems = refs[2 * count :]
    pairs = [(index_ref, index_scr), (slides_ref, slides_scr), (step_ref, step_scr), (states_ref, states_out)]
    copies = [pltpu.make_async_copy(x, y, sems.at[n]) for n, (x, y) in enumerate(pairs + list(zip(weights, outs)))]
    for copy in copies:
        copy.start()
    for copy in copies[:3]:
        copy.wait()
    times, frames = states_ref.shape[0], states_ref.shape[1]
    first_time = lax.axis_index("tm") * times
    for sweep in range(ITERS):
        offset = first_time if sweep == 0 else first_time + slides_scr[0]
        for i in range(times):
            index = index_scr[offset + i]
            picks_ref[ITERS + sweep * times + i] = index
            steps_ref[sweep * times + i] = step_scr[index]
        picks_ref[sweep] = slides_scr[sweep]
    copies[3].wait()
    for ref, first, end in ((low_ref, 0, 0), (high_ref, frames - HALO, frames - 1)):
        for t in range(times):
            ref[t * HALO : (t + 1) * HALO] = states_out[t, first : first + HALO].astype(BF)
        anchor = states_out[0, end]
        ref[times * HALO] = (anchor - anchor.astype(BF).astype(F32)).astype(BF)
    for copy in copies[4:]:
        copy.wait()


def silu_half(half):
    return half + half * jnp.tanh(half)


def embed_columns(sweep, inset, times, picks_ref, table_ref, last_scr):
    hidden, steps = table_ref.shape
    full = steps // LANES
    if steps % LANES:
        last_scr[:, : steps % LANES] = table_ref[:, full * LANES :]
    lane = lax.broadcasted_iota(jnp.int32, (1, LANES), 1)
    embed = jnp.zeros((hidden, LANES), F32)
    for slot in range(sweep * times, (sweep + 1) * times):
        index = picks_ref[ITERS + slot]
        tile = index // LANES
        start = pl.multiple_of(jnp.minimum(tile, full - 1) * LANES, LANES)
        block = table_ref[:, pl.ds(start, LANES)]
        if steps % LANES:
            block = jnp.where(tile == full, last_scr[...], block)
        place = index - tile * LANES
        shift = lax.rem(inset + slot + LANES - place, LANES)
        embed = jnp.where(lane == inset + slot, pltpu.roll(block, shift, 1), embed)
    embed = embed * 0.5
    rounded = embed.astype(BF).astype(F32)
    return (rounded + pltpu.roll(embed - rounded, EXTRA // 2, 1)).astype(BF)


def pack_weights(picks_ref, spatial_ref, temporal_ref, table_ref, spatial_out, temporal_out, project_ref, project_out, last_scr):
    hidden = spatial_out.shape[0]
    taps = spatial_ref.shape[0]
    inset = taps % LANES
    times = EXTRA // 2 // ITERS
    spatial_out[:, taps - inset :] = embed_columns(0, inset, times, picks_ref, table_ref, last_scr)
    weight = (spatial_ref[...].astype(F32) * 0.5).T.astype(BF)
    spatial_out[:, : taps - inset] = weight[:, : taps - inset]
    spatial_out[:, taps - inset : taps] = weight[:, taps - inset :]
    for lag in range(3):
        temporal_out[:, lag * hidden : (lag + 1) * hidden] = temporal_ref[lag] * 0.5
    for ref, used in ((temporal_out, 3 * hidden), (project_out, hidden)):
        if used < ref.shape[1]:
            ref[:, used:] = jnp.zeros((ref.shape[0], ref.shape[1] - used), BF)
    project_out[:, :hidden] = project_ref[...]


def columns_of(latent, valid, slot):
    cells = HEIGHT * WIDTH
    lane = lax.broadcasted_iota(jnp.int32, (1, cells), 1)
    col = lane % WIDTH
    zero = jnp.zeros_like(latent)
    left = jnp.where(col > 0, pltpu.roll(latent, 1, 1), zero)
    right = jnp.where(col < WIDTH - 1, pltpu.roll(latent, cells - 1, 1), zero)
    middle = (left, latent, right)
    above = [jnp.where(lane >= WIDTH, pltpu.roll(x, WIDTH, 1), zero) for x in middle]
    below = [jnp.where(lane < cells - WIDTH, pltpu.roll(x, cells - WIDTH, 1), zero) for x in middle]
    row = lax.broadcasted_iota(jnp.int32, (EXTRA, cells), 0)
    picks = jnp.where(lax.rem(row, EXTRA // 2) == slot, valid, 0.0).astype(BF)
    return jnp.concatenate([*above, *middle, *below, picks], axis=0)


def filled(parts, width):
    rows = sum(x.shape[0] for x in parts)
    if rows < TILE:
        parts = [*parts, jnp.zeros((TILE - rows, width), BF)]
    return parts[0] if len(parts) == 1 else jnp.concatenate(parts, axis=0)


def stage(sweep, items, latent_of, valid_of, put_first, first_at, add_drift, have,
          steps_ref, spatial_ref, temporal_ref, project_ref, aside=None):
    times = EXTRA // 2 // ITERS
    hidden = spatial_ref.shape[0]
    pieces = hidden // PIECE
    units = range(2)
    halves = [slice(q * TILE, (q + 1) * TILE) for q in units]
    order, needed = [], []
    for t, frame in items:
        for f in (frame - 1, frame, frame + 1):
            if (t, f) not in order and f not in have:
                order.append((t, f))
        needed.append(len(order))
    last = len(items) - 1

    def run(*accs):
        per = 3 * pieces + 1
        sets = [[[accs[q * per + k * pieces + i] for i in range(pieces)] for q in units] for k in range(3)]
        small = [accs[q * per + 3 * pieces] for q in units]
        state = {"pass": 0, "issued": 0}

        def one_pass(tiles, outs, lhs_of):
            register = state["pass"] % 2
            state["pass"] += 1
            for q in units:
                pltpu.matmul_push_rhs(tiles[q], staging_register=register, mxu_index=q)
            for i in range(len(outs[0])):
                lhs = lhs_of(i)
                for q in units:
                    pltpu.matmul_acc_lhs(outs[q][i], lhs, load_staged_rhs=register if i == 0 else None)

        def conv(into):
            t, f = order[state["issued"]]
            state["issued"] += 1
            columns = columns_of(latent_of(t, f), valid_of(f), sweep * times + t)
            tiles = [filled([columns[:, h]], TILE) for h in halves]
            one_pass(tiles, sets[into], lambda i: spatial_ref[i * PIECE : (i + 1) * PIECE, :])
            return t, f, into

        def finish_conv(t, f, into):
            for i in range(pieces):
                for q in units:
                    value = silu_half(pltpu.matmul_pop(sets[into][q][i])).astype(BF)
                    put_first(t, f, value, i * PIECE, halves[q])

        def temporal(n, k):
            t, frame = items[n]
            low, high = k * TILE, min((k + 1) * TILE, 3 * hidden)
            tiles = []
            for h in halves:
                parts = []
                for d in range(3):
                    start, stop = max(low, d * hidden), min(high, (d + 1) * hidden)
                    if start < stop:
                        parts.append(first_at(t, frame - 1 + d, start - d * hidden, stop - d * hidden, h))
                tiles.append(filled(parts, TILE))
            one_pass(tiles, sets[n % 2], lambda i: temporal_ref[i * PIECE : (i + 1) * PIECE, low : low + TILE])

        def finish_temporal(n):
            return [[silu_half(pltpu.matmul_pop(sets[n % 2][q][i])).astype(BF) for i in range(pieces)] for q in units]

        def project(second, k):
            count = TILE // PIECE
            tiles = [filled(second[q][k * count : (k + 1) * count], TILE) for q in units]
            one_pass(tiles, [[x] for x in small], lambda i: project_ref[:, k * TILE : (k + 1) * TILE])

        def finish_project(n):
            t, frame = items[n]
            for q in units:
                add_drift(t, frame, steps_ref[sweep * times + t] * pltpu.matmul_pop(small[q]), halves[q])

        temporal_passes = pl.cdiv(3 * hidden, TILE)
        project_passes = pl.cdiv(hidden, TILE)
        assert temporal_passes == 4 and project_passes == 2
        pending = None
        for i in range(needed[0]):
            issued = conv(2 if (needed[0] - 1 - i) % 2 == 0 else 1)
            if pending is not None:
                finish_conv(*pending)
            pending = issued
        second = None
        for n in range(len(items)):
            ahead = needed[min(n + 2, last)]
            temporal(n, 0)
            if pending is not None:
                finish_conv(*pending)
                pending = None
            early = conv(2) if state["issued"] < ahead else None
            temporal(n, 1)
            if n > 0:
                second = finish_temporal(n - 1)
            if n > 1:
                finish_project(n - 2)
            temporal(n, 2)
            if n == len(items) // 2 and aside is not None:
                aside()
            if n > 0:
                project(second, 0)
            if early is not None:
                finish_conv(*early)
            pending = conv(2) if state["issued"] < ahead else None
            temporal(n, 3)
            if n > 0:
                project(second, 1)
            assert n == last or state["issued"] >= needed[n + 1]
        second = finish_temporal(last)
        if last > 0:
            finish_project(last - 1)
        project(second, 0)
        project(second, 1)
        finish_project(last)

    shapes = [(PIECE, TILE)] * (3 * pieces) + [(project_ref.shape[0], TILE)]
    pl.run_scoped(run, *[pltpu.ACC(q)(dims, F32) for q in units for dims in shapes])


def edge_flag(frame, frames):
    slab = lax.axis_index("slab")
    if frame < 0:
        return jnp.where(slab > 0, 1.0, 0.0)
    if frame >= frames:
        return jnp.where(slab < lax.axis_size("slab") - 1, 1.0, 0.0)
    return 1.0


def inner_first(picks_ref, steps_ref, spatial_ref, temporal_ref, table_ref, out_weight_ref, states_ref,
                spatial_out, temporal_out, project_out, first_out, sums_out, last_scr):
    times, frames = states_ref.shape[0], states_ref.shape[1]
    hidden = temporal_out.shape[0]
    rank = lax.axis_index("tm")
    pack_weights(picks_ref, spatial_ref, temporal_ref, table_ref, spatial_out, temporal_out, out_weight_ref, project_out, last_scr)
    for frame in range(1, frames - 1):
        sums_out[0, frame - 1] = jnp.where(rank == 0, states_ref[0, frame], 0.0)

    def put_first(t, f, value, row, half):
        first_out[t, f * hidden + row : f * hidden + row + PIECE, half] = value

    def first_at(t, f, start, stop, half):
        return first_out[t, f * hidden + start : f * hidden + stop, half]

    def add_drift(t, frame, step, half):
        sums_out[t + 1, frame - 1, :, half] = sums_out[t, frame - 1, :, half] + step

    stage(0, [(t, f) for t in range(times) for f in range(1, frames - 1)],
          lambda t, f: states_ref[t, f].astype(BF), lambda f: 1.0, put_first, first_at, add_drift, (),
          steps_ref, spatial_out, temporal_out, project_out)


def deliver(slide, times, frame, sums_of, own_ref, send_ref):
    rank = lax.axis_index("tm")
    for j in range(times):
        own_ref[j, frame] = sums_of(jnp.minimum(j + slide, times))
        late = jnp.clip(j + slide - times, 0, times)
        sent = sums_of(jnp.where(rank == 0, times, late))
        send_ref[j, frame] = sent.astype(send_ref.dtype)
        if send_ref.shape[0] > times and j == 0:
            send_ref[times, frame] = (sent - sent.astype(BF).astype(F32)).astype(BF)


def outer_first(picks_ref, steps_ref, spatial_ref, temporal_ref, out_weight_ref, table_ref, states_ref,
                left_ref, right_ref, first_ref, inner_ref,
                own_ref, send_ref, later_ref, first_scr, sums_scr, last_scr):
    times, frames = states_ref.shape[0], states_ref.shape[1]
    hidden = temporal_ref.shape[0]
    rank = lax.axis_index("tm")
    outs = [-1, 0, frames - 1, frames]
    halo = [-2, -1, frames, frames + 1]

    def latent_of(t, f):
        return left_ref[t * HALO + f + HALO] if f < 0 else right_ref[t * HALO + f - frames]

    for n, f in enumerate(outs):
        if 0 <= f < frames:
            state = states_ref[0, f]
        else:
            rest = left_ref if f < 0 else right_ref
            state = latent_of(0, f).astype(F32) + rest[times * HALO].astype(F32)
        sums_scr[0, n] = jnp.where(rank == 0, state, 0.0)

    def put_first(t, f, value, row, half):
        start = halo.index(f) * hidden + row
        first_scr[t, start : start + PIECE, half] = value

    def first_at(t, f, start, stop, half):
        if f in halo:
            n = halo.index(f)
            return first_scr[t, n * hidden + start : n * hidden + stop, half]
        return first_ref[t, f * hidden + start : f * hidden + stop, half]

    def add_drift(t, frame, step, half):
        n = outs.index(frame)
        sums_scr[t + 1, n, :, half] = sums_scr[t, n, :, half] + step

    def next_embeddings():
        taps = 9 * states_ref.shape[2]
        inset = taps % LANES
        columns = embed_columns(1, inset, times, picks_ref, table_ref, last_scr)
        lane = lax.broadcasted_iota(jnp.int32, (1, LANES), 1)
        later_ref[:, : taps - inset] = spatial_ref[:, : taps - inset]
        later_ref[:, taps - inset :] = jnp.where(lane < inset, spatial_ref[:, taps - inset :], columns)

    stage(0, [(t, f) for t in range(times) for f in outs],
          latent_of, lambda f: edge_flag(f, frames), put_first, first_at, add_drift, range(frames),
          steps_ref, spatial_ref, temporal_ref, out_weight_ref, next_embeddings)
    for f in range(-1, frames + 1):
        sums = (lambda k, n=outs.index(f): sums_scr[k, n]) if f in outs else (lambda k, f=f: inner_ref[k, f - 1])
        deliver(picks_ref[0], times, f + 1, sums, own_ref, send_ref)


def second(picks_ref, steps_ref, spatial_ref, temporal_ref, out_weight_ref, mine_ref, other_ref,
           own_ref, send_ref, first_scr, sums_scr):
    times, frames = own_ref.shape[0], own_ref.shape[1]
    hidden = temporal_ref.shape[0]
    rank = lax.axis_index("tm")

    def state_of(t, f):
        rest = other_ref[times, f + 1].astype(F32)
        if t > 0:
            rest = rest * jnp.where(rank == 0, 0.0, 1.0)
        return mine_ref[t, f + 1] + (other_ref[t, f + 1].astype(F32) + rest)

    def latent_of(t, f):
        state = state_of(t, f)
        return (state if 0 <= f < frames else state * edge_flag(f, frames)).astype(BF)

    for f in range(frames):
        sums_scr[0, f] = jnp.where(rank == 0, state_of(0, f), 0.0)

    def put_first(t, f, value, row, half):
        start = (f + 1) * hidden + row
        first_scr[t, start : start + PIECE, half] = value

    def first_at(t, f, start, stop, half):
        return first_scr[t, (f + 1) * hidden + start : (f + 1) * hidden + stop, half]

    def add_drift(t, frame, step, half):
        sums_scr[t + 1, frame, :, half] = sums_scr[t, frame, :, half] + step

    stage(1, [(t, f) for t in range(times) for f in range(frames)],
          latent_of, lambda f: edge_flag(f, frames), put_first, first_at, add_drift, (),
          steps_ref, spatial_ref, temporal_ref, out_weight_ref)
    for f in range(frames):
        deliver(picks_ref[1], times, f, lambda k, f=f: sums_scr[k, f], own_ref, send_ref)


def local(window_states, spatial_weight, temporal_weight, out_weight, time_embed, step_size, time_index, slides):
    times, frames, channels, cells = window_states.shape
    hidden, taps = spatial_weight.shape
    slabs, ranks = lax.axis_size("slab"), lax.axis_size("tm")
    assert ranks == 2 and EXTRA == 2 * ITERS * times and hidden % PIECE == 0
    assert taps - taps % LANES + LANES == TILE and frames >= 3 and cells == HEIGHT * WIDTH
    plane = (channels, cells)
    weights = (spatial_weight.T, temporal_weight, time_embed.T, out_weight)
    edge = pltpu.VMEM((times * HALO + 1,) + plane, BF)
    *weights, states, low, high, picks, steps = pl.pallas_call(
        load,
        out_shape=(
            *[pltpu.VMEM(x.shape, x.dtype) for x in weights],
            pltpu.VMEM(window_states.shape, F32), edge, edge,
            pltpu.SMEM((ITERS * (times + 1),), jnp.int32), pltpu.SMEM((ITERS * times,), F32),
        ),
        in_specs=[HBM] * (4 + len(weights)),
        out_specs=(*[VMEM] * (3 + len(weights)), SMEM, SMEM),
        scratch_shapes=[
            pltpu.SMEM(time_index.shape, jnp.int32), pltpu.SMEM(slides.shape, jnp.int32),
            pltpu.SMEM(step_size.shape, F32), pltpu.SemaphoreType.DMA((4 + len(weights),)),
        ],
        compiler_params=pltpu.CompilerParams(vmem_limit_bytes=8 * MIB),
        name="load",
    )(*[kept(x, pltpu.HBM) for x in (window_states, time_index, slides, step_size, *weights)])
    spatial, temporal, table, project = weights
    scalars = (picks, steps)
    from_left = lax.ppermute(high, "slab", [(i, i + 1) for i in range(slabs - 1)])
    from_right = lax.ppermute(low, "slab", [(i + 1, i) for i in range(slabs - 1)])
    spatial, temporal, project, firsts, inner = call(
        inner_first, "inner_first",
        (
            ((hidden, TILE), BF),
            ((hidden, pl.cdiv(3 * hidden, TILE) * TILE), BF),
            ((channels, pl.cdiv(hidden, TILE) * TILE), BF),
            ((times, frames * hidden, cells), BF),
            ((times + 1, frames - 2) + plane, F32),
        ),
        scalars, (spatial, temporal, table, project, states),
        [pltpu.VMEM((hidden, LANES), F32)], 16,
    )
    wide = ((times, frames + 2) + plane, F32)
    mine, sent, later = call(
        outer_first, "outer_first", (wide, ((times + 1, frames + 2) + plane, BF), ((hidden, TILE), BF)), scalars,
        (spatial, temporal, project, table, states, from_left, from_right, firsts, inner),
        [
            pltpu.VMEM((times, 4 * hidden, cells), BF), pltpu.VMEM((times + 1, 4) + plane, F32),
            pltpu.VMEM((hidden, LANES), F32),
        ], 16,
    )
    swap = [(0, 1), (1, 0)]
    other = lax.ppermute(sent, "tm", swap)
    block = ((times, frames) + plane, F32)
    mine, sent = call(
        second, "second", (block, block), scalars, (later, temporal, project, mine, other),
        [pltpu.VMEM((times, (frames + 2) * hidden, cells), BF), pltpu.VMEM((times + 1, frames) + plane, F32)], 24,
    )
    return mine + lax.ppermute(sent, "tm", swap)


def solution(mesh):
    return jax.shard_map(
        local,
        mesh=mesh,
        in_specs=(
            P("tm", ("groups", "slab"), None, None),
            P(), P(), P(), P(), P(),
            P("groups"),
            P("groups"),
        ),
        out_specs=P("tm", ("groups", "slab"), None, None),
        check_vma=False,
    )
```

```python
import jax
import jax.numpy as jnp
from jax import lax
from jax.experimental import pallas as pl
from jax.experimental.pallas import tpu as pltpu
from jax.sharding import PartitionSpec as P

HEIGHT = 16
WIDTH = 32
ITERS = 2
HALO = 2
LANES = 128
EXTRA = 16
BF = jnp.bfloat16
F32 = jnp.float32
MIB = 1 << 20
TILE = 256
PIECE = 64
VMEM = pl.BlockSpec(memory_space=pltpu.VMEM)
SMEM = pl.BlockSpec(memory_space=pltpu.SMEM)
HBM = pl.BlockSpec(memory_space=pltpu.HBM)


def kept(x, space=pltpu.VMEM):
    return pltpu.with_memory_space_constraint(x, space)


def call(body, name, outs, scalars, arrays, scratch, limit):
    return pl.pallas_call(
        body,
        out_shape=tuple(pltpu.VMEM(dims, dtype) for dims, dtype in outs),
        in_specs=[SMEM] * len(scalars) + [VMEM] * len(arrays),
        out_specs=tuple(VMEM for _ in outs),
        scratch_shapes=scratch,
        compiler_params=pltpu.CompilerParams(vmem_limit_bytes=limit * MIB),
        name=name,
    )(*[kept(x, pltpu.SMEM) for x in scalars], *[kept(x) for x in arrays])


def load(states_ref, index_ref, slides_ref, step_ref, *refs):
    count = (len(refs) - 9) // 2
    weights, outs = refs[:count], refs[count : 2 * count]
    states_out, low_ref, high_ref, picks_ref, steps_ref, index_scr, slides_scr, step_scr, sems = refs[2 * count :]
    pairs = [(index_ref, index_scr), (slides_ref, slides_scr), (step_ref, step_scr), (states_ref, states_out)]
    copies = [pltpu.make_async_copy(x, y, sems.at[n]) for n, (x, y) in enumerate(pairs + list(zip(weights, outs)))]
    for copy in copies:
        copy.start()
    for copy in copies[:3]:
        copy.wait()
    times, frames = states_ref.shape[0], states_ref.shape[1]
    first_time = lax.axis_index("tm") * times
    for sweep in range(ITERS):
        offset = first_time if sweep == 0 else first_time + slides_scr[0]
        for i in range(times):
            index = index_scr[offset + i]
            picks_ref[ITERS + sweep * times + i] = index
            steps_ref[sweep * times + i] = step_scr[index]
        picks_ref[sweep] = slides_scr[sweep]
    copies[3].wait()
    for ref, first, end in ((low_ref, 0, 0), (high_ref, frames - HALO, frames - 1)):
        for t in range(times):
            ref[t * HALO : (t + 1) * HALO] = states_out[t, first : first + HALO].astype(BF)
        anchor = states_out[0, end]
        ref[times * HALO] = (anchor - anchor.astype(BF).astype(F32)).astype(BF)
    for copy in copies[4:]:
        copy.wait()


def silu_half(half):
    return half + half * jnp.tanh(half)


def embed_columns(sweep, inset, times, picks_ref, table_ref, last_scr):
    hidden, steps = table_ref.shape
    full = steps // LANES
    if steps % LANES:
        last_scr[:, : steps % LANES] = table_ref[:, full * LANES :]
    lane = lax.broadcasted_iota(jnp.int32, (1, LANES), 1)
    embed = jnp.zeros((hidden, LANES), F32)
    for slot in range(sweep * times, (sweep + 1) * times):
        index = picks_ref[ITERS + slot]
        tile = index // LANES
        start = pl.multiple_of(jnp.minimum(tile, full - 1) * LANES, LANES)
        block = table_ref[:, pl.ds(start, LANES)]
        if steps % LANES:
            block = jnp.where(tile == full, last_scr[...], block)
        place = index - tile * LANES
        shift = lax.rem(inset + slot + LANES - place, LANES)
        embed = jnp.where(lane == inset + slot, pltpu.roll(block, shift, 1), embed)
    embed = embed * 0.5
    rounded = embed.astype(BF).astype(F32)
    return (rounded + pltpu.roll(embed - rounded, EXTRA // 2, 1)).astype(BF)


def pack_weights(picks_ref, spatial_ref, temporal_ref, table_ref, spatial_out, temporal_out, project_ref, project_out, last_scr):
    hidden = spatial_out.shape[0]
    taps = spatial_ref.shape[0]
    inset = taps % LANES
    times = EXTRA // 2 // ITERS
    spatial_out[:, taps - inset :] = embed_columns(0, inset, times, picks_ref, table_ref, last_scr)
    weight = (spatial_ref[...].astype(F32) * 0.5).T.astype(BF)
    spatial_out[:, : taps - inset] = weight[:, : taps - inset]
    spatial_out[:, taps - inset : taps] = weight[:, taps - inset :]
    for lag in range(3):
        temporal_out[:, lag * hidden : (lag + 1) * hidden] = temporal_ref[lag] * 0.5
    for ref, used in ((temporal_out, 3 * hidden), (project_out, hidden)):
        if used < ref.shape[1]:
            ref[:, used:] = jnp.zeros((ref.shape[0], ref.shape[1] - used), BF)
    project_out[:, :hidden] = project_ref[...]


def columns_of(latent, valid, slot):
    cells = HEIGHT * WIDTH
    lane = lax.broadcasted_iota(jnp.int32, (1, cells), 1)
    col = lane % WIDTH
    zero = jnp.zeros_like(latent)
    left = jnp.where(col > 0, pltpu.roll(latent, 1, 1), zero)
    right = jnp.where(col < WIDTH - 1, pltpu.roll(latent, cells - 1, 1), zero)
    middle = (left, latent, right)
    above = [jnp.where(lane >= WIDTH, pltpu.roll(x, WIDTH, 1), zero) for x in middle]
    below = [jnp.where(lane < cells - WIDTH, pltpu.roll(x, cells - WIDTH, 1), zero) for x in middle]
    row = lax.broadcasted_iota(jnp.int32, (EXTRA, cells), 0)
    picks = jnp.where(lax.rem(row, EXTRA // 2) == slot, valid, 0.0).astype(BF)
    return jnp.concatenate([*above, *middle, *below, picks], axis=0)


def filled(parts, width):
    rows = sum(x.shape[0] for x in parts)
    if rows < TILE:
        parts = [*parts, jnp.zeros((TILE - rows, width), BF)]
    return parts[0] if len(parts) == 1 else jnp.concatenate(parts, axis=0)


def stage(sweep, items, latent_of, valid_of, put_first, first_at, add_drift, have,
          steps_ref, spatial_ref, temporal_ref, project_ref, aside=None):
    times = EXTRA // 2 // ITERS
    hidden = spatial_ref.shape[0]
    pieces = hidden // PIECE
    units = range(2)
    halves = [slice(q * TILE, (q + 1) * TILE) for q in units]
    order, needed = [], []
    for t, frame in items:
        for f in (frame - 1, frame, frame + 1):
            if (t, f) not in order and f not in have:
                order.append((t, f))
        needed.append(len(order))
    last = len(items) - 1

    def run(*accs):
        per = 3 * pieces + 1
        sets = [[[accs[q * per + k * pieces + i] for i in range(pieces)] for q in units] for k in range(3)]
        small = [accs[q * per + 3 * pieces] for q in units]
        state = {"pass": 0, "issued": 0}

        def one_pass(tiles, outs, lhs_of):
            register = state["pass"] % 2
            state["pass"] += 1
            for q in units:
                pltpu.matmul_push_rhs(tiles[q], staging_register=register, mxu_index=q)
            for i in range(len(outs[0])):
                lhs = lhs_of(i)
                for q in units:
                    pltpu.matmul_acc_lhs(outs[q][i], lhs, load_staged_rhs=register if i == 0 else None)

        def conv(into):
            t, f = order[state["issued"]]
            state["issued"] += 1
            columns = columns_of(latent_of(t, f), valid_of(f), sweep * times + t)
            tiles = [filled([columns[:, h]], TILE) for h in halves]
            one_pass(tiles, sets[into], lambda i: spatial_ref[i * PIECE : (i + 1) * PIECE, :])
            return t, f, into

        def finish_conv(t, f, into):
            for i in range(pieces):
                for q in units:
                    value = silu_half(pltpu.matmul_pop(sets[into][q][i])).astype(BF)
                    put_first(t, f, value, i * PIECE, halves[q])

        def temporal(n, k):
            t, frame = items[n]
            low, high = k * TILE, min((k + 1) * TILE, 3 * hidden)
            tiles = []
            for h in halves:
                parts = []
                for d in range(3):
                    start, stop = max(low, d * hidden), min(high, (d + 1) * hidden)
                    if start < stop:
                        parts.append(first_at(t, frame - 1 + d, start - d * hidden, stop - d * hidden, h))
                tiles.append(filled(parts, TILE))
            one_pass(tiles, sets[n % 2], lambda i: temporal_ref[i * PIECE : (i + 1) * PIECE, low : low + TILE])

        def finish_temporal(n):
            return [[silu_half(pltpu.matmul_pop(sets[n % 2][q][i])).astype(BF) for i in range(pieces)] for q in units]

        def project(second, k):
            count = TILE // PIECE
            tiles = [filled(second[q][k * count : (k + 1) * count], TILE) for q in units]
            one_pass(tiles, [[x] for x in small], lambda i: project_ref[:, k * TILE : (k + 1) * TILE])

        def finish_project(n):
            t, frame = items[n]
            for q in units:
                add_drift(t, frame, steps_ref[sweep * times + t] * pltpu.matmul_pop(small[q]), halves[q])

        temporal_passes = pl.cdiv(3 * hidden, TILE)
        project_passes = pl.cdiv(hidden, TILE)
        assert temporal_passes == 4 and project_passes == 2
        pending = None
        for i in range(needed[0]):
            issued = conv(2 if (needed[0] - 1 - i) % 2 == 0 else 1)
            if pending is not None:
                finish_conv(*pending)
            pending = issued
        second = None
        for n in range(len(items)):
            ahead = needed[min(n + 2, last)]
            temporal(n, 0)
            if pending is not None:
                finish_conv(*pending)
                pending = None
            early = conv(2) if state["issued"] < ahead else None
            temporal(n, 1)
            if n > 0:
                second = finish_temporal(n - 1)
            if n > 1:
                finish_project(n - 2)
            temporal(n, 2)
            if n == len(items) // 2 and aside is not None:
                aside()
            if n > 0:
                project(second, 0)
            if early is not None:
                finish_conv(*early)
            pending = conv(2) if state["issued"] < ahead else None
            temporal(n, 3)
            if n > 0:
                project(second, 1)
            assert n == last or state["issued"] >= needed[n + 1]
        second = finish_temporal(last)
        if last > 0:
            finish_project(last - 1)
        project(second, 0)
        project(second, 1)
        finish_project(last)

    shapes = [(PIECE, TILE)] * (3 * pieces) + [(project_ref.shape[0], TILE)]
    pl.run_scoped(run, *[pltpu.ACC(q)(dims, F32) for q in units for dims in shapes])


def edge_flag(frame, frames):
    slab = lax.axis_index("slab")
    if frame < 0:
        return jnp.where(slab > 0, 1.0, 0.0)
    if frame >= frames:
        return jnp.where(slab < lax.axis_size("slab") - 1, 1.0, 0.0)
    return 1.0


def inner_first(picks_ref, steps_ref, spatial_ref, temporal_ref, table_ref, out_weight_ref, states_ref,
                spatial_out, temporal_out, project_out, first_out, sums_out, last_scr):
    times, frames = states_ref.shape[0], states_ref.shape[1]
    hidden = temporal_out.shape[0]
    rank = lax.axis_index("tm")
    pack_weights(picks_ref, spatial_ref, temporal_ref, table_ref, spatial_out, temporal_out, out_weight_ref, project_out, last_scr)
    for frame in range(1, frames - 1):
        sums_out[0, frame - 1] = jnp.where(rank == 0, states_ref[0, frame], 0.0)

    def put_first(t, f, value, row, half):
        first_out[t, f * hidden + row : f * hidden + row + PIECE, half] = value

    def first_at(t, f, start, stop, half):
        return first_out[t, f * hidden + start : f * hidden + stop, half]

    def add_drift(t, frame, step, half):
        sums_out[t + 1, frame - 1, :, half] = sums_out[t, frame - 1, :, half] + step

    stage(0, [(t, f) for t in range(times) for f in range(1, frames - 1)],
          lambda t, f: states_ref[t, f].astype(BF), lambda f: 1.0, put_first, first_at, add_drift, (),
          steps_ref, spatial_out, temporal_out, project_out)


def deliver(slide, times, frame, sums_of, own_ref, send_ref):
    rank = lax.axis_index("tm")
    for j in range(times):
        own_ref[j, frame] = sums_of(jnp.minimum(j + slide, times))
        late = jnp.clip(j + slide - times, 0, times)
        sent = sums_of(jnp.where(rank == 0, times, late))
        send_ref[j, frame] = sent.astype(send_ref.dtype)
        if send_ref.shape[0] > times and j == 0:
            send_ref[times, frame] = (sent - sent.astype(BF).astype(F32)).astype(BF)


def outer_first(picks_ref, steps_ref, spatial_ref, temporal_ref, out_weight_ref, table_ref, states_ref,
                left_ref, right_ref, first_ref, inner_ref,
                own_ref, send_ref, later_ref, first_scr, sums_scr, last_scr):
    times, frames = states_ref.shape[0], states_ref.shape[1]
    hidden = temporal_ref.shape[0]
    rank = lax.axis_index("tm")
    outs = [-1, 0, frames - 1, frames]
    halo = [-2, -1, frames, frames + 1]

    def latent_of(t, f):
        return left_ref[t * HALO + f + HALO] if f < 0 else right_ref[t * HALO + f - frames]

    for n, f in enumerate(outs):
        if 0 <= f < frames:
            state = states_ref[0, f]
        else:
            rest = left_ref if f < 0 else right_ref
            state = latent_of(0, f).astype(F32) + rest[times * HALO].astype(F32)
        sums_scr[0, n] = jnp.where(rank == 0, state, 0.0)

    def put_first(t, f, value, row, half):
        start = halo.index(f) * hidden + row
        first_scr[t, start : start + PIECE, half] = value

    def first_at(t, f, start, stop, half):
        if f in halo:
            n = halo.index(f)
            return first_scr[t, n * hidden + start : n * hidden + stop, half]
        return first_ref[t, f * hidden + start : f * hidden + stop, half]

    def add_drift(t, frame, step, half):
        n = outs.index(frame)
        sums_scr[t + 1, n, :, half] = sums_scr[t, n, :, half] + step

    def next_embeddings():
        taps = 9 * states_ref.shape[2]
        inset = taps % LANES
        columns = embed_columns(1, inset, times, picks_ref, table_ref, last_scr)
        lane = lax.broadcasted_iota(jnp.int32, (1, LANES), 1)
        later_ref[:, : taps - inset] = spatial_ref[:, : taps - inset]
        later_ref[:, taps - inset :] = jnp.where(lane < inset, spatial_ref[:, taps - inset :], columns)

    stage(0, [(t, f) for t in range(times) for f in outs],
          latent_of, lambda f: edge_flag(f, frames), put_first, first_at, add_drift, range(frames),
          steps_ref, spatial_ref, temporal_ref, out_weight_ref, next_embeddings)
    for f in range(-1, frames + 1):
        sums = (lambda k, n=outs.index(f): sums_scr[k, n]) if f in outs else (lambda k, f=f: inner_ref[k, f - 1])
        deliver(picks_ref[0], times, f + 1, sums, own_ref, send_ref)


def second(picks_ref, steps_ref, spatial_ref, temporal_ref, out_weight_ref, mine_ref, other_ref,
           own_ref, send_ref, first_scr, sums_scr):
    times, frames = own_ref.shape[0], own_ref.shape[1]
    hidden = temporal_ref.shape[0]
    rank = lax.axis_index("tm")

    def state_of(t, f):
        rest = other_ref[times, f + 1].astype(F32)
        if t > 0:
            rest = rest * jnp.where(rank == 0, 0.0, 1.0)
        return mine_ref[t, f + 1] + (other_ref[t, f + 1].astype(F32) + rest)

    def latent_of(t, f):
        state = state_of(t, f)
        return (state if 0 <= f < frames else state * edge_flag(f, frames)).astype(BF)

    for f in range(frames):
        sums_scr[0, f] = jnp.where(rank == 0, state_of(0, f), 0.0)

    def put_first(t, f, value, row, half):
        start = (f + 1) * hidden + row
        first_scr[t, start : start + PIECE, half] = value

    def first_at(t, f, start, stop, half):
        return first_scr[t, (f + 1) * hidden + start : (f + 1) * hidden + stop, half]

    def add_drift(t, frame, step, half):
        sums_scr[t + 1, frame, :, half] = sums_scr[t, frame, :, half] + step

    stage(1, [(t, f) for t in range(times) for f in range(frames)],
          latent_of, lambda f: edge_flag(f, frames), put_first, first_at, add_drift, (),
          steps_ref, spatial_ref, temporal_ref, out_weight_ref)
    for f in range(frames):
        deliver(picks_ref[1], times, f, lambda k, f=f: sums_scr[k, f], own_ref, send_ref)


def combine(mine_ref, other_ref, out_ref, sum_scr, sems):
    copies = []
    for j in range(mine_ref.shape[0]):
        sum_scr[j] = mine_ref[j] + other_ref[j]
        copy = pltpu.make_async_copy(sum_scr.at[j], out_ref.at[j], sems.at[j])
        copy.start()
        copies.append(copy)
    for copy in copies:
        copy.wait()


def local(window_states, spatial_weight, temporal_weight, out_weight, time_embed, step_size, time_index, slides):
    times, frames, channels, cells = window_states.shape
    hidden, taps = spatial_weight.shape
    slabs, ranks = lax.axis_size("slab"), lax.axis_size("tm")
    assert ranks == 2 and EXTRA == 2 * ITERS * times and hidden % PIECE == 0
    assert taps - taps % LANES + LANES == TILE and frames >= 3 and cells == HEIGHT * WIDTH
    plane = (channels, cells)
    weights = (spatial_weight.T, temporal_weight, time_embed.T, out_weight)
    edge = pltpu.VMEM((times * HALO + 1,) + plane, BF)
    *weights, states, low, high, picks, steps = pl.pallas_call(
        load,
        out_shape=(
            *[pltpu.VMEM(x.shape, x.dtype) for x in weights],
            pltpu.VMEM(window_states.shape, F32), edge, edge,
            pltpu.SMEM((ITERS * (times + 1),), jnp.int32), pltpu.SMEM((ITERS * times,), F32),
        ),
        in_specs=[HBM] * (4 + len(weights)),
        out_specs=(*[VMEM] * (3 + len(weights)), SMEM, SMEM),
        scratch_shapes=[
            pltpu.SMEM(time_index.shape, jnp.int32), pltpu.SMEM(slides.shape, jnp.int32),
            pltpu.SMEM(step_size.shape, F32), pltpu.SemaphoreType.DMA((4 + len(weights),)),
        ],
        compiler_params=pltpu.CompilerParams(vmem_limit_bytes=8 * MIB),
        name="load",
    )(*[kept(x, pltpu.HBM) for x in (window_states, time_index, slides, step_size, *weights)])
    spatial, temporal, table, project = weights
    scalars = (picks, steps)
    from_left = lax.ppermute(high, "slab", [(i, i + 1) for i in range(slabs - 1)])
    from_right = lax.ppermute(low, "slab", [(i + 1, i) for i in range(slabs - 1)])
    spatial, temporal, project, firsts, inner = call(
        inner_first, "inner_first",
        (
            ((hidden, TILE), BF),
            ((hidden, pl.cdiv(3 * hidden, TILE) * TILE), BF),
            ((channels, pl.cdiv(hidden, TILE) * TILE), BF),
            ((times, frames * hidden, cells), BF),
            ((times + 1, frames - 2) + plane, F32),
        ),
        scalars, (spatial, temporal, table, project, states),
        [pltpu.VMEM((hidden, LANES), F32)], 16,
    )
    wide = ((times, frames + 2) + plane, F32)
    mine, sent, later = call(
        outer_first, "outer_first", (wide, ((times + 1, frames + 2) + plane, BF), ((hidden, TILE), BF)), scalars,
        (spatial, temporal, project, table, states, from_left, from_right, firsts, inner),
        [
            pltpu.VMEM((times, 4 * hidden, cells), BF), pltpu.VMEM((times + 1, 4) + plane, F32),
            pltpu.VMEM((hidden, LANES), F32),
        ], 16,
    )
    swap = [(0, 1), (1, 0)]
    other = lax.ppermute(sent, "tm", swap)
    block = ((times, frames) + plane, F32)
    mine, sent = call(
        second, "second", (block, block), scalars, (later, temporal, project, mine, other),
        [pltpu.VMEM((times, (frames + 2) * hidden, cells), BF), pltpu.VMEM((times + 1, frames) + plane, F32)], 24,
    )
    other = lax.ppermute(sent, "tm", swap)
    return pl.pallas_call(
        combine,
        out_shape=jax.ShapeDtypeStruct(window_states.shape, F32),
        in_specs=[VMEM, VMEM],
        out_specs=HBM,
        scratch_shapes=[pltpu.VMEM(window_states.shape, F32), pltpu.SemaphoreType.DMA((times,))],
        compiler_params=pltpu.CompilerParams(vmem_limit_bytes=4 * MIB),
        name="combine",
    )(kept(mine), kept(other))


def solution(mesh):
    return jax.shard_map(
        local,
        mesh=mesh,
        in_specs=(
            P("tm", ("groups", "slab"), None, None),
            P(), P(), P(), P(), P(),
            P("groups"),
            P("groups"),
        ),
        out_specs=P("tm", ("groups", "slab"), None, None),
        check_vma=False,
    )
```
